32 devices in a mesh: groups: 2 (over y), gx: 16 (over z, x, core).
Axes of the slice: x: 2, y: 2, z: 4, core: 2. Of those that a mesh axis runs over, the one named last changes fastest.
Arguments:
- stream_in: bfloat16 [32, 8192], P(('groups', 'gx')), parts along dimension 0, may hold values from -6 to 6
- query: bfloat16 [32, 8192], P(('groups', 'gx')), parts along dimension 0, may hold values from -4.5 to 4.5
- key_new: bfloat16 [32, 1024], P(('groups', 'gx')), parts along dimension 0, may hold values from -4.5 to 4.5
- value_new: bfloat16 [32, 1024], P(('groups', 'gx')), parts along dimension 0, may hold values from -6 to 6
- key_cache: bfloat16 [32, 128, 1024], P(('groups', 'gx')), parts along dimension 0, may hold values from -6 to 6
- value_cache: bfloat16 [32, 128, 1024], P(('groups', 'gx')), parts along dimension 0, may hold values from -6 to 6
- lengths: int32 [32], P(('groups', 'gx')), parts along dimension 0, may hold values from 1 to 128, as said below
- route_ids: int32 [32, 2], P(('groups', 'gx')), parts along dimension 0, may hold values from 0 to 3, as said below
- route_scores: float32 [32, 2], P(('groups', 'gx')), parts along dimension 0, may hold values from -6 to 6
- out_weight: bfloat16 [8192, 8192], P(None, 'gx'), may hold values from -0.0625 to 0.0625
- norm_gain: float32 [8192], replicated, may hold values from 0.1 to 1.9
- gate_weight: bfloat16 [2, 16384, 7168], P(None, 'gx'), may hold values from -0.0625 to 0.0625
- up_weight: bfloat16 [2, 16384, 7168], P(None, 'gx'), may hold values from -0.0625 to 0.0625
- down_weight: bfloat16 [2, 114688, 1024], P(None, 'gx'), may hold values from -0.046875 to 0.046875
Outputs:
- layer_out: bfloat16 [32, 8192], P(('groups', 'gx')), parts along dimension 0
The draws below stay inside these ranges and needn't reach their ends.
There are 2 independent parts, one for each index of `groups`. The reference program is written for one: setup_inputs(seed, part) draws one part's arguments, and reference() takes and returns one part's arrays. A program takes and returns all parts, laid end to end along the dimension named above; an argument that names none is the same for every part. Nothing has to cross between parts.
Inputs may be any that keep to these rules, and one draw needn't show every extreme that they name: `lengths`: 1 to 128; some sequence fills all 128 slots. `route_ids`: each row names two different experts of 0 to 3; in one replica's batch each of the experts 0 and 1 is named by at most 10 sequences, and one of them by exactly 10.
All inputs are finite; a program needn't handle non-finite values.
Results may differ from the reference program's by a relative error of at most 0.0095.
Values may be sent and summed in bfloat16 or wider, within the bound.
No kernel may reach another device: no remote copies, remote signals or barrier semaphores. Data moves between devices by JAX's collectives and lax.ppermute only.
A program may use at most 192 MiB of HBM per device.

```python
import jax
import jax.numpy as jnp
from jax import lax

D = 8192
NH = 64
KVH = 8
HS = 128
H = 14336
RESIDENT = 2
MSPLIT = 8
CTX = 128
HSPLIT = 2
BATCH = 16


def shared_heads(key):
    base = jax.random.fold_in(key, 71)
    key_q, key_k = jax.random.split(base, 2)
    queries = jnp.clip(jax.random.normal(key_q, (BATCH, NH, HS), jnp.float32), -4.5, 4.5)
    keys = jnp.clip(jax.random.normal(key_k, (BATCH, KVH, HS), jnp.float32), -4.5, 4.5)
    return (queries.reshape(BATCH, NH * HS), keys.reshape(BATCH, KVH * HS))


def draw_query(key, part):
    return shared_heads(key)[0].astype(jnp.bfloat16)


def draw_key_new(key, part):
    return shared_heads(key)[1].astype(jnp.bfloat16)


def draw_lengths(key, part):
    key_len, key_full = jax.random.split(jax.random.fold_in(key, 5))
    filled = jax.random.randint(key_len, (BATCH,), 1, CTX + 1)
    chosen = jax.random.randint(key_full, (), 0, BATCH)
    return jnp.where(jnp.arange(BATCH) == chosen, CTX, filled).astype(jnp.int32)


def draw_route_ids(key, part):
    keys = jax.random.split(jax.random.fold_in(key, 9), 6)
    limit = 5 * BATCH // 8
    rank_a = jax.random.permutation(keys[0], BATCH)
    other_count = jax.random.randint(keys[1], (), BATCH // 4, limit + 1)
    rank_b = jax.random.permutation(keys[2], BATCH)
    in_a = rank_a < limit
    in_b = rank_b < other_count
    flip = jax.random.randint(keys[3], (), 0, 2)
    in_zero = jnp.where(flip == 0, in_a, in_b)
    in_one = jnp.where(flip == 0, in_b, in_a)
    spare = 2 + jax.random.randint(keys[4], (BATCH,), 0, 2)
    first = jnp.where(in_zero, 0, jnp.where(in_one, 1, 2))
    second = jnp.where(in_zero & in_one, 1, jnp.where(in_zero | in_one, spare, 3))
    order = jax.random.randint(keys[5], (BATCH,), 0, 2) == 1
    left = jnp.where(order, second, first)
    right = jnp.where(order, first, second)
    return jnp.stack([left, right], axis=-1).astype(jnp.int32)


def shard_levels(key, extent, pieces, smallest, largest):
    def one(dim, shards_of):
        steps = jax.random.uniform(jax.random.fold_in(jax.random.fold_in(key, 6), dim), (shards_of,), jnp.float32, smallest / len(pieces), largest / len(pieces))
        return jnp.repeat(jnp.exp(steps), extent[dim] // shards_of).reshape((-1,) + (1,) * (len(extent) - dim - 1))

    gain = one(*pieces[0])
    for cut in pieces[1:]:
        gain = gain * one(*cut)
    return gain


def noise(rng, dims, scale, reach, cuts=(), kind=jnp.bfloat16):
    array = scale * jax.random.normal(rng, dims, jnp.float32)
    if cuts:
        array = array * shard_levels(rng, dims, cuts, -0.22, 0.18)
    return jnp.clip(array, -reach, reach).astype(kind)


def setup_inputs(seed: int = 0, part: int = 0) -> dict:
    arg_keys = jax.random.split(jax.random.key(seed), 15)
    part_splits = jax.random.split(jax.random.fold_in(arg_keys[14], part), 15)
    return {
        "stream_in": noise(part_splits[0], (BATCH, D), 1.0, 6.0, ((0, 16),)),
        "query": draw_query(jax.random.fold_in(jax.random.fold_in(arg_keys[14], part), 71), part),
        "key_new": draw_key_new(jax.random.fold_in(jax.random.fold_in(arg_keys[14], part), 71), part),
        "value_new": noise(part_splits[3], (BATCH, KVH * HS), 1.0, 6.0, ((0, 16),)),
        "key_cache": noise(part_splits[4], (BATCH, CTX, KVH * HS), 1.0, 6.0, ((0, 16),)),
        "value_cache": noise(part_splits[5], (BATCH, CTX, KVH * HS), 1.0, 6.0, ((0, 16),)),
        "lengths": draw_lengths(jax.random.fold_in(jax.random.fold_in(arg_keys[14], part), 71), part),
        "route_ids": draw_route_ids(jax.random.fold_in(jax.random.fold_in(arg_keys[14], part), 71), part),
        "route_scores": noise(part_splits[8], (BATCH, 2), 1.0, 6.0, ((0, 16),), jnp.float32),
        "out_weight": noise(arg_keys[9], (NH * HS, D), (NH * HS) ** -0.5, 0.0625, ((1, 16),)),
        "norm_gain": jnp.clip(1.0 + 0.18 * jax.random.normal(arg_keys[10], (D,), jnp.float32), 0.1, 1.9),
        "gate_weight": noise(arg_keys[11], (RESIDENT, HSPLIT * D, H // HSPLIT), D ** -0.5, 0.0625, ((1, 16),)),
        "up_weight": noise(arg_keys[12], (RESIDENT, HSPLIT * D, H // HSPLIT), D ** -0.5, 0.0625, ((1, 16),)),
        "down_weight": noise(arg_keys[13], (RESIDENT, MSPLIT * H, D // MSPLIT), H ** -0.5, 0.046875, ((1, 16),)),
    }


def attend_one(items):
    query_row, key_row, value_row, key_slots, value_slots, length = items
    group = NH // KVH
    scale = HS ** (-0.5)
    q_four = query_row.astype(jnp.float32).reshape(KVH, group, HS)
    k_own = key_row.astype(jnp.float32).reshape(KVH, HS)
    v_own = value_row.astype(jnp.float32).reshape(KVH, HS)
    k_all = key_slots.astype(jnp.float32).reshape(CTX, KVH, HS)
    v_all = value_slots.astype(jnp.float32).reshape(CTX, KVH, HS)
    scores = jnp.einsum('kgd,ckd->kgc', q_four, k_all) * scale
    live = jnp.arange(CTX, dtype=jnp.int32) < length
    scores = jnp.where(live[None, None, :], scores, -1e+30)
    own = jnp.einsum('kgd,kd->kg', q_four, k_own) * scale
    top = jnp.maximum(lax.optimization_barrier(jnp.max(scores, axis=-1)), own)
    e_cache = jnp.exp(scores - top[:, :, None])
    e_own = jnp.exp(own - top)
    total = lax.optimization_barrier(jnp.sum(e_cache, axis=-1)) + e_own
    p_cache = (e_cache / total[:, :, None]).astype(jnp.bfloat16)
    p_own = (e_own / total).astype(jnp.bfloat16)
    mixed = jnp.einsum('kgc,ckd->kgd', p_cache.astype(jnp.float32), v_all)
    mixed = mixed + p_own.astype(jnp.float32)[:, :, None] * v_own[:, None, :]
    return mixed.reshape(NH * HS).astype(jnp.bfloat16)

def reference(stream_in, query, key_new, value_new, key_cache, value_cache, lengths, route_ids, route_scores, out_weight, norm_gain, gate_weight, up_weight, down_weight):
    gate_full = gate_weight.reshape(RESIDENT, MSPLIT, HSPLIT, D // MSPLIT, H // HSPLIT).transpose(0, 1, 3, 2, 4).reshape(RESIDENT, D, H)
    up_full = up_weight.reshape(RESIDENT, MSPLIT, HSPLIT, D // MSPLIT, H // HSPLIT).transpose(0, 1, 3, 2, 4).reshape(RESIDENT, D, H)
    down_full = down_weight.reshape(RESIDENT, MSPLIT, HSPLIT, H // HSPLIT, D // MSPLIT).transpose(0, 2, 3, 1, 4).reshape(RESIDENT, H, D)
    attn = lax.map(attend_one, (query, key_new, value_new, key_cache, value_cache, lengths))
    proj = jnp.dot(attn, out_weight, preferred_element_type=jnp.float32).astype(jnp.bfloat16)
    resid = stream_in.astype(jnp.float32) + proj.astype(jnp.float32)
    power = lax.optimization_barrier(jnp.mean(resid * resid, axis=-1, keepdims=True))
    normed = (resid * lax.rsqrt(power + 1e-05) * norm_gain).astype(jnp.bfloat16)
    probs = jax.nn.softmax(route_scores, axis=-1)
    columns = []
    for expert in range(RESIDENT):
        columns.append(lax.optimization_barrier(jnp.sum(jnp.where(route_ids == expert, probs, 0.0), axis=-1)))
    weight = jnp.stack(columns, axis=-1).astype(jnp.bfloat16)
    ffn = jnp.zeros(resid.shape, jnp.float32)
    for expert in range(RESIDENT):
        gate = jnp.dot(normed, gate_full[expert], preferred_element_type=jnp.float32)
        upper = jnp.dot(normed, up_full[expert], preferred_element_type=jnp.float32)
        hidden = (jax.nn.silu(gate) * upper).astype(jnp.bfloat16)
        result = jnp.dot(hidden, down_full[expert], preferred_element_type=jnp.float32)
        ffn = ffn + weight[:, expert].astype(jnp.float32)[:, None] * result
    return (resid + ffn).astype(jnp.bfloat16)
```

```python
import functools

import jax
import jax.numpy as jnp
from jax import lax
from jax.experimental import pallas as pl
from jax.experimental.pallas import tpu as pltpu
from jax.sharding import PartitionSpec as P

NH = 64
KVH = 8
HS = 128
RESIDENT = 2
MSPLIT = 8
HINT = 100_000_000_000


def partner(value, axis, distance):
    return lax.ppermute(value, axis, [(i, i ^ 1 << distance) for i in range(lax.axis_size(axis))])


def attend_local(query, key_new, value_new, key_cache, value_cache, lengths):
    seqs = query.shape[0]
    slots = key_cache.shape[1]
    group = NH // KVH
    scale = HS ** (-0.5)
    q_four = query.reshape(seqs, KVH, group, HS)
    k_all = key_cache.reshape(seqs, slots, KVH, HS)
    v_all = value_cache.reshape(seqs, slots, KVH, HS)
    k_own = key_new.reshape(seqs, KVH, HS)
    v_own = value_new.reshape(seqs, KVH, HS)
    scores = (
        jnp.einsum("skgd,sckd->skgc", q_four, k_all, preferred_element_type=jnp.float32) * scale
    )
    live = jnp.arange(slots, dtype=jnp.int32)[None, :] < lengths[:, None]
    scores = jnp.where(live[:, None, None, :], scores, -1e30)
    own = jnp.einsum("skgd,skd->skg", q_four, k_own, preferred_element_type=jnp.float32) * scale
    top = jnp.maximum(jnp.max(scores, axis=-1), own)
    e_cache = jnp.exp(scores - top[..., None])
    e_own = jnp.exp(own - top)
    total = jnp.sum(e_cache, axis=-1) + e_own
    p_cache = (e_cache / total[..., None]).astype(jnp.bfloat16)
    p_own = (e_own / total).astype(jnp.bfloat16)
    mixed = jnp.einsum("skgc,sckd->skgd", p_cache, v_all, preferred_element_type=jnp.float32)
    mixed = mixed + p_own.astype(jnp.float32)[..., None] * v_own.astype(jnp.float32)[:, :, None, :]
    return mixed.reshape(seqs, NH * HS).astype(jnp.bfloat16)


def gated(parts):
    return (jax.nn.silu(parts[..., 0, :]) * parts[..., 1, :]).astype(jnp.bfloat16)


def plain_on_device(
    stream_in,
    query,
    key_new,
    value_new,
    key_cache,
    value_cache,
    lengths,
    route_ids,
    route_scores,
    out_weight,
    norm_gain,
    gate_weight,
    up_weight,
    down_weight,
):
    seqs = stream_in.shape[0]
    width = stream_in.shape[1]
    members = lax.axis_size("gx")
    batch = seqs * members
    hsplit = members // MSPLIT
    low_bits = hsplit.bit_length() - 1
    model_bits = MSPLIT.bit_length() - 1
    place = lax.axis_index("gx")
    model_block = place // hsplit
    block_width = width // MSPLIT
    hidden_cols = gate_weight.shape[2]
    narrow = hidden_cols // MSPLIT
    attn = attend_local(query, key_new, value_new, key_cache, value_cache, lengths)
    proj_cols = jnp.dot(
        lax.all_gather(attn, "gx", axis=0, tiled=True),
        out_weight,
        preferred_element_type=jnp.float32,
    ).astype(jnp.bfloat16)
    proj = lax.all_to_all(proj_cols, "gx", split_axis=0, concat_axis=1, tiled=True)
    resid = stream_in.astype(jnp.float32) + proj.astype(jnp.float32)
    power = jnp.mean(resid * resid, axis=-1, keepdims=True)
    normed = (resid * lax.rsqrt(power + 1e-05) * norm_gain).astype(jnp.bfloat16)
    probs = jax.nn.softmax(route_scores, axis=-1)
    columns = []
    for expert in range(RESIDENT):
        columns.append(jnp.sum(jnp.where(route_ids == expert, probs, 0.0), axis=-1))
    weight = jnp.stack(columns, axis=-1).astype(jnp.bfloat16)
    normed_all, weight_all = (
        lax.all_gather(normed, "gx", axis=0, tiled=True),
        lax.all_gather(weight, "gx", axis=0, tiled=True),
    )
    rows_in = lax.dynamic_slice_in_dim(normed_all, model_block * block_width, block_width, 1)
    gate_view = gate_weight.reshape(RESIDENT, block_width, MSPLIT, narrow)
    up_view = up_weight.reshape(RESIDENT, block_width, MSPLIT, narrow)
    gate_part = jnp.einsum("bd,rdpc->bprc", rows_in, gate_view, preferred_element_type=jnp.float32)
    up_part = jnp.einsum("bd,rdpc->bprc", rows_in, up_view, preferred_element_type=jnp.float32)
    parts = jnp.stack([gate_part, up_part], axis=3)
    for bit in range(model_bits):
        parts = parts + partner(parts.astype(jnp.bfloat16), "gx", low_bits + bit).astype(
            parts.dtype
        )
    hidden = gated(parts)
    down_view = down_weight.reshape(RESIDENT, MSPLIT, narrow, block_width)
    scales = weight_all.astype(jnp.float32)
    result = jnp.zeros((batch, block_width), jnp.float32)
    for expert in range(RESIDENT):
        term = jnp.einsum(
            "bpc,pcn->bn",
            hidden[:, :, expert],
            down_view[expert],
            preferred_element_type=jnp.float32,
        )
        result = result + scales[:, expert][:, None] * term
    partial_out = result.reshape(members, seqs, block_width)
    got = lax.all_to_all(
        partial_out.astype(jnp.bfloat16), "gx", split_axis=0, concat_axis=0, tiled=True
    ).astype(partial_out.dtype)
    got = jnp.sum(got.reshape(MSPLIT, hsplit, seqs, block_width), axis=1)
    ffn = got.transpose(1, 0, 2).reshape(seqs, width)
    return (resid + ffn).astype(jnp.bfloat16)


def lane_iota(shape):
    return lax.broadcasted_iota(jnp.int32, shape, len(shape) - 1)


def row_iota(shape):
    return lax.broadcasted_iota(jnp.int32, shape, 0)


def split_three(value):
    high = value.astype(jnp.bfloat16)
    rest = value - high.astype(jnp.float32)
    mid = rest.astype(jnp.bfloat16)
    low = (rest - mid.astype(jnp.float32)).astype(jnp.bfloat16)
    return high, mid, low


def one_block(kernel, outs, args, spaces, name, scratch=(), flops=0, grant=3 << 20):
    return pl.pallas_call(
        kernel,
        out_shape=[jax.ShapeDtypeStruct(shape, dtype) for shape, dtype in outs],
        in_specs=[pl.BlockSpec(memory_space=space) for space in spaces],
        out_specs=[pl.BlockSpec(memory_space=pltpu.VMEM) for _ in outs],
        scratch_shapes=list(scratch),
        cost_estimate=pl.CostEstimate(flops=flops, transcendentals=0, bytes_accessed=1 << 20),
        compiler_params=pltpu.CompilerParams(vmem_limit_bytes=grant),
        name=name,
    )(*args)


def attend_kernel(*refs):
    lengths, sources, out, places, sems, work = refs[0], refs[1:9], refs[9], refs[10:18], refs[18], refs[19:]
    copies = [
        pltpu.make_async_copy(source, place, sems.at[i])
        for i, (source, place) in enumerate(zip(sources, places))
    ]
    for copy in copies:
        copy.start()
    for copy in copies:
        copy.wait()
    ids, scores_in, query, key_new, value_new, stream, keys, values = places
    q_rows, s_rows, own_k, own_v, s_acc = work
    blocks, rows = out.shape[0], out.shape[1]
    group = NH // KVH
    for head in range(NH):
        q_rows[head : head + 1, :] = query[0:1, head * HS : (head + 1) * HS].astype(jnp.float32)
    for tile in range(s_rows.shape[0]):
        s_rows[tile : tile + 1, :] = stream[0:1, tile * HS : (tile + 1) * HS].astype(jnp.float32)
    for g in range(KVH):
        cut = slice(g * HS, (g + 1) * HS)
        here = slice(g * group, (g + 1) * group)
        own_k[here, :] = jnp.broadcast_to(key_new[0:1, cut].astype(jnp.float32), (group, HS))
        own_v[here, :] = jnp.broadcast_to(value_new[0:1, cut].astype(jnp.float32), (group, HS))
        s_acc[here, :] = lax.dot_general(
            q_rows[here, :].astype(jnp.bfloat16),
            keys[0, :, cut],
            (((1,), (1,)), ((), ())),
            preferred_element_type=jnp.float32,
        )
    scale = HS ** (-0.5)
    scores = s_acc[...] * scale
    scores = jnp.where(lane_iota(scores.shape) < lengths[0], scores, -1e30)
    own = jnp.sum(q_rows[...] * own_k[...], axis=-1, keepdims=True) * scale
    top = jnp.maximum(jnp.max(scores, axis=-1, keepdims=True), own)
    e_cache = jnp.exp(scores - top)
    e_own = jnp.exp(own - top)
    total = jnp.sum(e_cache, axis=-1, keepdims=True) + e_own
    p_cache = e_cache / total
    p_own = (e_own / total).astype(jnp.bfloat16).astype(jnp.float32)
    s_acc[...] = p_cache
    for g in range(KVH):
        cut = slice(g * HS, (g + 1) * HS)
        here = slice(g * group, (g + 1) * group)
        mixed = jnp.dot(
            s_acc[here, :].astype(jnp.bfloat16), values[0, :, cut], preferred_element_type=jnp.float32
        )
        q_rows[here, :] = mixed + p_own[here, :] * own_v[here, :]
    attn = q_rows[...].astype(jnp.bfloat16)
    first = jnp.full((8, HS), scores_in[0, 0])
    second = jnp.full((8, HS), scores_in[0, 1])
    peak = jnp.maximum(first, second)
    e_first = jnp.exp(first - peak)
    e_second = jnp.exp(second - peak)
    both = e_first + e_second
    tail = jnp.zeros((8, HS), jnp.float32)
    for expert in range(RESIDENT):
        w = jnp.where(ids[0, 0] == expert, e_first / both, 0.0)
        w = w + jnp.where(ids[0, 1] == expert, e_second / both, 0.0)
        tail = jnp.where(row_iota(tail.shape) == expert, w, tail)
    tail = tail.astype(jnp.bfloat16)
    per = s_rows.shape[0] // blocks
    for block in range(blocks):
        out[block, 0:NH, :] = attn
        out[block, NH : NH + per, :] = s_rows[block * per : (block + 1) * per, :].astype(jnp.bfloat16)
        out[block, NH + per : rows, :] = tail


def project_kernel(weight, gathered, gain, out, resid_out, slot_out, pick_out, rows32, lhs, acc, *, slots):
    batch, width = acc.shape
    rows = gathered.shape[2]
    half = lax.axis_index("gx") % 2
    place = lax.axis_index("gx")
    rows32[...] = gathered[...].reshape(batch * rows, HS).astype(jnp.float32)
    for head in range(NH):
        lhs[:, head * HS : (head + 1) * HS] = rows32[pl.ds(head, batch, stride=rows), :].astype(jnp.bfloat16)
    acc[...] = jnp.dot(lhs[...], weight[...], preferred_element_type=jnp.float32)
    per = width // HS
    power = jnp.zeros((batch, 1), jnp.float32)
    for q in range(per):
        cut = slice(q * HS, (q + 1) * HS)
        stream = rows32[pl.ds(NH + half * per + q, batch, stride=rows), :]
        resid = stream + acc[:, cut].astype(jnp.bfloat16).astype(jnp.float32)
        resid_out[:, cut] = resid
        power = power + jnp.sum(resid * resid, axis=-1, keepdims=True)
        scaled = resid * gain[pl.ds(place * per + q, 1), :]
        out[:, cut] = scaled.astype(jnp.bfloat16)
    lanes = lane_iota((batch, HS))
    high, mid, low = split_three(jnp.broadcast_to(power, (batch, HS)))
    zero = jnp.zeros((batch, HS), jnp.float32)
    packed = jnp.where(lanes == 0, high.astype(jnp.float32), zero)
    packed = jnp.where(lanes == 1, mid.astype(jnp.float32), packed)
    packed = jnp.where(lanes == 2, low.astype(jnp.float32), packed)
    out[:, width : width + HS] = packed.astype(jnp.bfloat16)
    tri = (lane_iota((batch, batch)) < row_iota((batch, batch))).astype(jnp.bfloat16)
    onehot = jnp.zeros((batch, HS), jnp.float32)
    picked = jnp.zeros((batch, HS), jnp.float32)
    for expert in range(RESIDENT):
        w = rows32[pl.ds(NH + 2 * per + expert, batch, stride=rows), :]
        named = w > 0.0
        rank = jnp.dot(tri, named.astype(jnp.bfloat16), preferred_element_type=jnp.float32)
        slot = lanes.astype(jnp.float32)
        for turn, low_edge in enumerate((expert * 16 + expert * slots % 8, 32 + expert * slots)):
            inside = (lanes >= low_edge) & (lanes < low_edge + slots)
            hit = inside & named & (rank + float(low_edge) == slot)
            onehot = jnp.where(hit, 1.0, onehot)
            if turn == 0:
                picked = jnp.where(hit, w, picked)
    slot_out[...] = onehot
    pick_out[...] = picked


def merged(left, right):
    return jnp.concatenate([left[:8], left[8:] + right[:8], right[8:]], axis=0)


class UpBlocks:
    def __init__(self, up, ring, sems, side):
        self.up, self.ring, self.sems, self.side = up, ring, sems, side
        self.depth, self.rows, self.narrow = ring.shape
        self.pieces = up.shape[1] // self.rows
        self.total = 4 * RESIDENT * self.pieces
        for k in range(self.depth):
            self.copy(k).start()

    def columns(self, z, side):
        return pl.ds(pl.multiple_of((2 * z + side) * self.narrow, HS), self.narrow)

    def copy(self, k):
        slot = k % self.depth
        block, piece = k // self.pieces, k % self.pieces
        source = self.up.at[
            block % RESIDENT,
            piece * self.rows : (piece + 1) * self.rows,
            self.columns(block // RESIDENT, self.side),
        ]
        return pltpu.make_async_copy(source, self.ring.at[slot], self.sems.at[slot])

    def times(self, lhs, z, expert):
        result = None
        for piece in range(self.pieces):
            k = (z * RESIDENT + expert) * self.pieces + piece
            self.copy(k).wait()
            cut = slice(piece * self.rows, (piece + 1) * self.rows)
            term = jnp.dot(lhs[expert, :, cut], self.ring[k % self.depth], preferred_element_type=jnp.float32)
            result = term if result is None else result + term
            if k + self.depth < self.total:
                self.copy(k + self.depth).start()
        return result


def stacked(work, gate, up, half):
    work[0:half, :] = gate[:half]
    work[half : 2 * half, :] = up[:half]


def gate_kernel(mine, other, onehot, gate, up, out, gate_out, lhs_out, place_out, tail_out, ring, sems, work, *, slots):
    batch = mine.shape[0]
    place = lax.axis_index("gx")
    side = place // 2 % 2
    blocks = UpBlocks(up, ring, sems, 1 - side)
    lines = 2 * RESIDENT * slots
    width = mine.shape[1] - HS
    first = place % 2 == 0
    own = mine[:, :width].astype(jnp.float32)
    far = other[:, :width].astype(jnp.float32)
    left = jnp.where(first, own, far).astype(jnp.bfloat16)
    right = jnp.where(first, far, own).astype(jnp.bfloat16)
    hot = onehot[...].astype(jnp.bfloat16)
    over = (((0,), (0,)), ((), ()))
    for at, piece in ((0, left), (width, right)):
        spread = lax.dot_general(hot[:, : RESIDENT * 16], piece, over, preferred_element_type=jnp.float32)
        for expert in range(RESIDENT):
            lhs_out[expert, :, at : at + width] = spread[expert * 16 : (expert + 1) * 16].astype(jnp.bfloat16)
    power = mine[:, width:].astype(jnp.float32) + other[:, width:].astype(jnp.float32)
    power = jnp.sum(power, axis=-1, keepdims=True)
    eye = lane_iota((batch, HS)) == row_iota((batch, HS))
    line = jnp.sum(jnp.where(eye, power, 0.0), axis=0, keepdims=True)
    high, mid, low = split_three(line)
    rows = row_iota((8, HS))
    tail = jnp.where(rows == 0, high.astype(jnp.float32), 0.0)
    tail = jnp.where(rows == 1, mid.astype(jnp.float32), tail)
    tail = jnp.where(rows == 2, low.astype(jnp.float32), tail)
    tail_out[...] = tail
    hot_rows = hot[:, 32 : 32 + place_out.shape[0]]
    place_out[...] = lax.dot_general(hot_rows, eye.astype(jnp.bfloat16), over, preferred_element_type=jnp.float32)
    narrow = blocks.narrow
    half = RESIDENT * slots

    for z in range(out.shape[0]):
        out[z, out.shape[1] - 8 :, :] = tail.astype(jnp.bfloat16)
        cut = slice(2 * z * narrow, 2 * (z + 1) * narrow)
        gates = merged(
            *[jnp.dot(lhs_out[expert], gate[expert, :, cut], preferred_element_type=jnp.float32) for expert in range(RESIDENT)]
        )
        lower, upper = gates[:, :narrow], gates[:, narrow:]
        gate_out[z] = jnp.where(side == 0, lower, upper)
        ups = [blocks.times(lhs_out, z, expert) for expert in range(RESIDENT)]
        stacked(work, jnp.where(side == 0, upper, lower), merged(*ups), half)
        for q in range(narrow // HS):
            out[z, q * lines : (q + 1) * lines, :] = work[:, q * HS : (q + 1) * HS].astype(jnp.bfloat16)


def up_kernel(lhs, tail, gate_sums, up, out, ring, sems, work, *, slots):
    side = lax.axis_index("gx") // 2 % 2
    blocks = UpBlocks(up, ring, sems, side)
    lines = 2 * RESIDENT * slots
    half = RESIDENT * slots
    for z in range(out.shape[0]):
        out[z, out.shape[1] - 8 :, :] = tail[...]
        ups = [blocks.times(lhs, z, expert) for expert in range(RESIDENT)]
        stacked(work, gate_sums[z], merged(*ups), half)
        for q in range(blocks.narrow // HS):
            out[z, q * lines : (q + 1) * lines, :] = work[:, q * HS : (q + 1) * HS]


def pair_kernel(near_sums, got, keep, *sends):
    z = lax.axis_index("gx") // 4
    keep[...] = near_sums[z] + got[z].astype(jnp.float32)
    for d, send in enumerate(sends, 1):
        send[...] = (near_sums[z ^ d] + got[z ^ d].astype(jnp.float32)).astype(jnp.bfloat16)


def gated_kernel(keep, first, second, third, place, out, work, packed, *, slots, width):
    lines = 2 * RESIDENT * slots
    blocks = out.shape[0]
    per = (keep.shape[0] - 8) // lines
    total = keep[...]
    for got in (first, second, third):
        total = total + got[...].astype(jnp.float32)
    work[...] = total
    line = jnp.sum(work[per * lines : per * lines + 8, :], axis=0, keepdims=True)
    inverse = lax.rsqrt(line / width + 1e-05)
    factor = jnp.sum(place[...] * inverse, axis=-1, keepdims=True)
    half = RESIDENT * slots
    scale = factor[:half, :]
    packed[packed.shape[0] - 8 :, :] = jnp.zeros((8, HS), jnp.float32)
    for q in range(per):
        gate = work[q * lines : q * lines + half, :] * scale
        up = work[q * lines + half : (q + 1) * lines, :] * scale
        packed[q * half : (q + 1) * half, :] = gate / (1.0 + jnp.exp(-gate)) * up
    hidden = packed[...].astype(jnp.bfloat16)
    for block in range(blocks):
        out[block] = hidden


def down_kernel(hidden, down, picked, resid, out, spread, rows32, lhs, acc, *, slots):
    blocks = hidden.shape[0]
    half = lax.axis_index("gx") % 2
    each = RESIDENT * slots
    per = lhs.shape[2] // blocks // HS
    for block in range(blocks):
        rows32[block] = hidden[block].astype(jnp.float32)
        for q in range(per):
            at = (block * per + q) * HS
            for expert in range(RESIDENT):
                start = q * each + expert * slots // 8 * 8
                lhs[expert, :, at : at + HS] = rows32[block, start : start + 16, :].astype(jnp.bfloat16)
    tile = acc.shape[1] // 2

    def columns(k, carry):
        cut = pl.ds(pl.multiple_of(k * tile, tile), tile)
        for expert in range(RESIDENT):
            acc[expert * 16 : (expert + 1) * 16, cut] = jnp.dot(
                lhs[expert], down[expert, :, cut], preferred_element_type=jnp.float32
            )
        return carry

    lax.fori_loop(0, 2, columns, 0)
    weight = picked[...].astype(jnp.bfloat16)[:, : RESIDENT * 16]
    result = None
    for part in split_three(acc[...]):
        term = jnp.dot(weight, part, preferred_element_type=jnp.float32)
        result = term if result is None else result + term
    own = resid[...]
    none = jnp.zeros_like(own)
    width = own.shape[1]
    result = result + jnp.concatenate(
        [jnp.where(half == 0, own, none), jnp.where(half == 0, none, own)], axis=1
    )
    tiles = result.shape[1] // HS
    for q in range(tiles):
        for h in range(2):
            spread[pl.ds(h * tiles + q, blocks, stride=2 * tiles), :] = result[
                h * blocks : (h + 1) * blocks, q * HS : (q + 1) * HS
            ]
    out[...] = spread[...].reshape(out.shape).astype(jnp.bfloat16)


def finish_kernel(got, out):
    blocks = got.shape[0] // 2
    per = got.shape[1]
    for block in range(blocks):
        total = got[2 * block].astype(jnp.float32) + got[2 * block + 1].astype(jnp.float32)
        for q in range(per):
            at = (block * per + q) * HS
            out[0:1, at : at + HS] = total[q : q + 1, :].astype(jnp.bfloat16)


def fast_on_device(
    stream_in,
    query,
    key_new,
    value_new,
    key_cache,
    value_cache,
    lengths,
    route_ids,
    route_scores,
    out_weight,
    norm_gain,
    gate_weight,
    up_weight,
    down_weight,
):
    width = stream_in.shape[1]
    members = lax.axis_size("gx")
    batch = members
    own_width = width // members
    block_width = width // MSPLIT
    hidden_cols = gate_weight.shape[2]
    slots = 5 * batch // 8
    lines = 2 * RESIDENT * slots
    bf16, f32 = jnp.bfloat16, jnp.float32
    chips = [[2 * chip + core for chip in range(MSPLIT)] for core in range(2)]
    cores = [[2 * chip, 2 * chip + 1] for chip in range(MSPLIT)]
    swap = [(i, i ^ 1) for i in range(members)]
    V = pltpu.VMEM

    def near(value):
        return pltpu.with_memory_space_constraint(value, V)

    rows = NH + block_width // HS + 8

    def exchange(value, groups):
        return lax.all_to_all(
            value, "gx", split_axis=0, concat_axis=0, tiled=True, axis_index_groups=groups
        )

    loaded = (route_ids, route_scores, query, key_new, value_new, stream_in, key_cache, value_cache)
    (sent,) = one_block(
        attend_kernel,
        [((MSPLIT, rows, HS), bf16)],
        [lengths] + [pltpu.with_memory_space_constraint(value, pltpu.HBM) for value in loaded],
        [pltpu.SMEM] + [pltpu.HBM] * len(loaded),
        "attend",
        scratch=[(pltpu.SMEM if i < 2 else pltpu.VMEM)(value.shape, value.dtype) for i, value in enumerate(loaded)]
        + [pltpu.SemaphoreType.DMA((len(loaded),))]
        + [
            pltpu.VMEM((NH, HS), f32),
            pltpu.VMEM((width // HS, HS), f32),
            pltpu.VMEM((NH, HS), f32),
            pltpu.VMEM((NH, HS), f32),
            pltpu.VMEM((NH, HS), f32),
        ],
        flops=HINT,
    )
    chip_rows = exchange(sent, chips)
    gathered = lax.all_gather(chip_rows, "gx", axis=0, tiled=False, axis_index_groups=cores)
    mine, resid, onehot, picked = one_block(
        functools.partial(project_kernel, slots=slots),
        [((batch, own_width + HS), bf16), ((batch, own_width), f32), ((batch, HS), f32), ((batch, HS), f32)],
        (near(out_weight), gathered, norm_gain.reshape(width // HS, HS)),
        [V, V, V],
        "project",
        scratch=[
            pltpu.VMEM((batch * rows, HS), f32),
            pltpu.VMEM((batch, width), bf16),
            pltpu.VMEM((batch, own_width), f32),
        ],
    )
    other = lax.ppermute(mine, "gx", swap)
    narrow = hidden_cols // MSPLIT
    per = narrow // HS
    held = -(-RESIDENT * slots // 8) * 8
    chunk = (per * lines + 8, HS)
    flat = (-(-per * RESIDENT * slots // 8) * 8, HS)
    up_hbm = pltpu.with_memory_space_constraint(up_weight, pltpu.HBM)

    def side_scratch(depth):
        return [
            pltpu.VMEM((depth, block_width // 2, narrow), bf16),
            pltpu.SemaphoreType.DMA((depth,)),
            pltpu.VMEM((lines, narrow), f32),
        ]

    far, gate_sums, lhs, place, tail = one_block(
        functools.partial(gate_kernel, slots=slots),
        [
            ((4,) + chunk, bf16),
            ((4, held, narrow), f32),
            ((RESIDENT, 16, block_width), bf16),
            ((held, HS), f32),
            ((8, HS), f32),
        ],
        (near(mine), near(other), near(onehot), near(gate_weight), up_hbm),
        [V, V, V, V, pltpu.HBM],
        "gate",
        scratch=side_scratch(6),
        grant=7 << 20,
    )
    crossed = lax.ppermute(far, "gx", [(i, i ^ 2) for i in range(members)])
    (near_sums,) = one_block(
        functools.partial(up_kernel, slots=slots),
        [((4,) + chunk, f32)],
        (lhs, tail, gate_sums, up_hbm),
        [V, V, V, pltpu.HBM],
        "up",
        scratch=side_scratch(7),
        grant=8 << 20,
    )
    keep, *sends = one_block(
        pair_kernel, [(chunk, f32)] + [(chunk, bf16)] * 3, (near_sums, crossed), [V, V], "pair"
    )
    got = [lax.ppermute(sends[d - 1], "gx", [(i, i ^ 4 * d) for i in range(members)]) for d in (1, 2, 3)]
    (hidden,) = one_block(
        functools.partial(gated_kernel, slots=slots, width=width),
        [((MSPLIT,) + flat, bf16)],
        (keep, *got, place),
        [V] * 5,
        "gated",
        scratch=[pltpu.VMEM(chunk, f32), pltpu.VMEM(flat, f32)],
        flops=HINT,
    )
    hidden_all = exchange(hidden, chips)
    (partial_out,) = one_block(
        functools.partial(down_kernel, slots=slots),
        [((members, block_width // HS, HS), bf16)],
        (hidden_all, near(down_weight), picked, resid),
        [V, V, V, V],
        "down",
        scratch=[
            pltpu.VMEM((members * block_width // HS, HS), f32),
            pltpu.VMEM((MSPLIT,) + flat, f32),
            pltpu.VMEM((RESIDENT, 16, hidden_cols), bf16),
            pltpu.VMEM((RESIDENT * 16, block_width), f32),
        ],
    )
    last = exchange(partial_out, None)
    (out,) = one_block(finish_kernel, [((1, width), bf16)], (last,), [V], "finish")
    return out


def fits(shapes, members):
    width = shapes[0][1]
    hidden_cols = shapes[11][2]
    return (
        members == 2 * MSPLIT
        and shapes[0][0] == 1
        and shapes[4][1] == HS
        and width == NH * HS
        and width % (members * HS) == 0
        and hidden_cols % (MSPLIT * HS) == 0
        and (5 * members) % 8 == 0
        and 8 <= 5 * members // 8 <= 14
        and RESIDENT == 2
    )


def on_device(*args):
    if fits([arg.shape for arg in args], lax.axis_size("gx")):
        return fast_on_device(*args)
    return plain_on_device(*args)


def solution(mesh):
    return jax.shard_map(
        on_device,
        mesh=mesh,
        in_specs=(
            P(("groups", "gx"), None),
            P(("groups", "gx"), None),
            P(("groups", "gx"), None),
            P(("groups", "gx"), None),
            P(("groups", "gx"), None, None),
            P(("groups", "gx"), None, None),
            P(("groups", "gx")),
            P(("groups", "gx"), None),
            P(("groups", "gx"), None),
            P(None, "gx"),
            P(),
            P(None, "gx", None),
            P(None, "gx", None),
            P(None, "gx", None),
        ),
        out_specs=P(("groups", "gx"), None),
        check_vma=False,
    )
```

```python
import functools

import jax
import jax.numpy as jnp
from jax import lax
from jax.experimental import pallas as pl
from jax.experimental.pallas import tpu as pltpu
from jax.sharding import PartitionSpec as P

NH = 64
KVH = 8
HS = 128
RESIDENT = 2
MSPLIT = 8
HINT = 100_000_000_000


def partner(value, axis, distance):
    return lax.ppermute(value, axis, [(i, i ^ 1 << distance) for i in range(lax.axis_size(axis))])


def attend_local(query, key_new, value_new, key_cache, value_cache, lengths):
    seqs = query.shape[0]
    slots = key_cache.shape[1]
    group = NH // KVH
    scale = HS ** (-0.5)
    q_four = query.reshape(seqs, KVH, group, HS)
    k_all = key_cache.reshape(seqs, slots, KVH, HS)
    v_all = value_cache.reshape(seqs, slots, KVH, HS)
    k_own = key_new.reshape(seqs, KVH, HS)
    v_own = value_new.reshape(seqs, KVH, HS)
    scores = (
        jnp.einsum("skgd,sckd->skgc", q_four, k_all, preferred_element_type=jnp.float32) * scale
    )
    live = jnp.arange(slots, dtype=jnp.int32)[None, :] < lengths[:, None]
    scores = jnp.where(live[:, None, None, :], scores, -1e30)
    own = jnp.einsum("skgd,skd->skg", q_four, k_own, preferred_element_type=jnp.float32) * scale
    top = jnp.maximum(jnp.max(scores, axis=-1), own)
    e_cache = jnp.exp(scores - top[..., None])
    e_own = jnp.exp(own - top)
    total = jnp.sum(e_cache, axis=-1) + e_own
    p_cache = (e_cache / total[..., None]).astype(jnp.bfloat16)
    p_own = (e_own / total).astype(jnp.bfloat16)
    mixed = jnp.einsum("skgc,sckd->skgd", p_cache, v_all, preferred_element_type=jnp.float32)
    mixed = mixed + p_own.astype(jnp.float32)[..., None] * v_own.astype(jnp.float32)[:, :, None, :]
    return mixed.reshape(seqs, NH * HS).astype(jnp.bfloat16)


def gated(parts):
    return (jax.nn.silu(parts[..., 0, :]) * parts[..., 1, :]).astype(jnp.bfloat16)


def plain_on_device(
    stream_in,
    query,
    key_new,
    value_new,
    key_cache,
    value_cache,
    lengths,
    route_ids,
    route_scores,
    out_weight,
    norm_gain,
    gate_weight,
    up_weight,
    down_weight,
):
    seqs = stream_in.shape[0]
    width = stream_in.shape[1]
    members = lax.axis_size("gx")
    batch = seqs * members
    hsplit = members // MSPLIT
    low_bits = hsplit.bit_length() - 1
    model_bits = MSPLIT.bit_length() - 1
    place = lax.axis_index("gx")
    model_block = place // hsplit
    block_width = width // MSPLIT
    hidden_cols = gate_weight.shape[2]
    narrow = hidden_cols // MSPLIT
    attn = attend_local(query, key_new, value_new, key_cache, value_cache, lengths)
    proj_cols = jnp.dot(
        lax.all_gather(attn, "gx", axis=0, tiled=True),
        out_weight,
        preferred_element_type=jnp.float32,
    ).astype(jnp.bfloat16)
    proj = lax.all_to_all(proj_cols, "gx", split_axis=0, concat_axis=1, tiled=True)
    resid = stream_in.astype(jnp.float32) + proj.astype(jnp.float32)
    power = jnp.mean(resid * resid, axis=-1, keepdims=True)
    normed = (resid * lax.rsqrt(power + 1e-05) * norm_gain).astype(jnp.bfloat16)
    probs = jax.nn.softmax(route_scores, axis=-1)
    columns = []
    for expert in range(RESIDENT):
        columns.append(jnp.sum(jnp.where(route_ids == expert, probs, 0.0), axis=-1))
    weight = jnp.stack(columns, axis=-1).astype(jnp.bfloat16)
    normed_all, weight_all = (
        lax.all_gather(normed, "gx", axis=0, tiled=True),
        lax.all_gather(weight, "gx", axis=0, tiled=True),
    )
    rows_in = lax.dynamic_slice_in_dim(normed_all, model_block * block_width, block_width, 1)
    gate_view = gate_weight.reshape(RESIDENT, block_width, MSPLIT, narrow)
    up_view = up_weight.reshape(RESIDENT, block_width, MSPLIT, narrow)
    gate_part = jnp.einsum("bd,rdpc->bprc", rows_in, gate_view, preferred_element_type=jnp.float32)
    up_part = jnp.einsum("bd,rdpc->bprc", rows_in, up_view, preferred_element_type=jnp.float32)
    parts = jnp.stack([gate_part, up_part], axis=3)
    for bit in range(model_bits):
        parts = parts + partner(parts.astype(jnp.bfloat16), "gx", low_bits + bit).astype(
            parts.dtype
        )
    hidden = gated(parts)
    down_view = down_weight.reshape(RESIDENT, MSPLIT, narrow, block_width)
    scales = weight_all.astype(jnp.float32)
    result = jnp.zeros((batch, block_width), jnp.float32)
    for expert in range(RESIDENT):
        term = jnp.einsum(
            "bpc,pcn->bn",
            hidden[:, :, expert],
            down_view[expert],
            preferred_element_type=jnp.float32,
        )
        result = result + scales[:, expert][:, None] * term
    partial_out = result.reshape(members, seqs, block_width)
    got = lax.all_to_all(
        partial_out.astype(jnp.bfloat16), "gx", split_axis=0, concat_axis=0, tiled=True
    ).astype(partial_out.dtype)
    got = jnp.sum(got.reshape(MSPLIT, hsplit, seqs, block_width), axis=1)
    ffn = got.transpose(1, 0, 2).reshape(seqs, width)
    return (resid + ffn).astype(jnp.bfloat16)


def lane_iota(shape):
    return lax.broadcasted_iota(jnp.int32, shape, len(shape) - 1)


def row_iota(shape):
    return lax.broadcasted_iota(jnp.int32, shape, 0)


def split_three(value):
    high = value.astype(jnp.bfloat16)
    rest = value - high.astype(jnp.float32)
    mid = rest.astype(jnp.bfloat16)
    low = (rest - mid.astype(jnp.float32)).astype(jnp.bfloat16)
    return high, mid, low


def one_block(kernel, outs, args, spaces, name, scratch=(), flops=0, grant=3 << 20):
    return pl.pallas_call(
        kernel,
        out_shape=[jax.ShapeDtypeStruct(shape, dtype) for shape, dtype in outs],
        in_specs=[pl.BlockSpec(memory_space=space) for space in spaces],
        out_specs=[pl.BlockSpec(memory_space=pltpu.VMEM) for _ in outs],
        scratch_shapes=list(scratch),
        cost_estimate=pl.CostEstimate(flops=flops, transcendentals=0, bytes_accessed=1 << 20),
        compiler_params=pltpu.CompilerParams(vmem_limit_bytes=grant),
        name=name,
    )(*args)


def attend_kernel(*refs):
    lengths, sources, out, places, sems, work = refs[0], refs[1:9], refs[9], refs[10:18], refs[18], refs[19:]
    copies = [
        pltpu.make_async_copy(source, place, sems.at[i])
        for i, (source, place) in enumerate(zip(sources, places))
    ]
    for copy in copies:
        copy.start()
    for copy in copies:
        copy.wait()
    ids, scores_in, query, key_new, value_new, stream, keys, values = places
    q_rows, s_rows, own_k, own_v, s_acc = work
    blocks, rows = out.shape[0], out.shape[1]
    group = NH // KVH
    for head in range(NH):
        q_rows[head : head + 1, :] = query[0:1, head * HS : (head + 1) * HS].astype(jnp.float32)
    for tile in range(s_rows.shape[0]):
        s_rows[tile : tile + 1, :] = stream[0:1, tile * HS : (tile + 1) * HS].astype(jnp.float32)
    for g in range(KVH):
        cut = slice(g * HS, (g + 1) * HS)
        here = slice(g * group, (g + 1) * group)
        own_k[here, :] = jnp.broadcast_to(key_new[0:1, cut].astype(jnp.float32), (group, HS))
        own_v[here, :] = jnp.broadcast_to(value_new[0:1, cut].astype(jnp.float32), (group, HS))
        s_acc[here, :] = lax.dot_general(
            q_rows[here, :].astype(jnp.bfloat16),
            keys[0, :, cut],
            (((1,), (1,)), ((), ())),
            preferred_element_type=jnp.float32,
        )
    scale = HS ** (-0.5)
    scores = s_acc[...] * scale
    scores = jnp.where(lane_iota(scores.shape) < lengths[0], scores, -1e30)
    own = jnp.sum(q_rows[...] * own_k[...], axis=-1, keepdims=True) * scale
    top = jnp.maximum(jnp.max(scores, axis=-1, keepdims=True), own)
    e_cache = jnp.exp(scores - top)
    e_own = jnp.exp(own - top)
    total = jnp.sum(e_cache, axis=-1, keepdims=True) + e_own
    p_cache = e_cache / total
    p_own = (e_own / total).astype(jnp.bfloat16).astype(jnp.float32)
    s_acc[...] = p_cache
    for g in range(KVH):
        cut = slice(g * HS, (g + 1) * HS)
        here = slice(g * group, (g + 1) * group)
        mixed = jnp.dot(
            s_acc[here, :].astype(jnp.bfloat16), values[0, :, cut], preferred_element_type=jnp.float32
        )
        q_rows[here, :] = mixed + p_own[here, :] * own_v[here, :]
    attn = q_rows[...].astype(jnp.bfloat16)
    first = jnp.full((8, HS), scores_in[0, 0])
    second = jnp.full((8, HS), scores_in[0, 1])
    peak = jnp.maximum(first, second)
    e_first = jnp.exp(first - peak)
    e_second = jnp.exp(second - peak)
    both = e_first + e_second
    tail = jnp.zeros((8, HS), jnp.float32)
    for expert in range(RESIDENT):
        w = jnp.where(ids[0, 0] == expert, e_first / both, 0.0)
        w = w + jnp.where(ids[0, 1] == expert, e_second / both, 0.0)
        tail = jnp.where(row_iota(tail.shape) == expert, w, tail)
    tail = tail.astype(jnp.bfloat16)
    per = s_rows.shape[0] // blocks
    for block in range(blocks):
        out[block, 0:NH, :] = attn
        out[block, NH : NH + per, :] = s_rows[block * per : (block + 1) * per, :].astype(jnp.bfloat16)
        out[block, NH + per : rows, :] = tail


def project_kernel(weight, here, there, gain, out, resid_out, slot_out, pick_out, rows32, lhs, acc, *, slots):
    batch, width = acc.shape
    chips, rows = here.shape[:2]
    place = lax.axis_index("gx")
    half = place % 2
    for source, core in ((here, half), (there, 1 - half)):
        first = pl.multiple_of(core * (chips * rows), 8)
        rows32[pl.ds(first, chips * rows), :] = source[...].reshape(chips * rows, HS).astype(jnp.float32)
    for head in range(NH):
        lhs[:, head * HS : (head + 1) * HS] = rows32[pl.ds(head, batch, stride=rows), :].astype(jnp.bfloat16)
    acc[...] = jnp.dot(lhs[...], weight[...], preferred_element_type=jnp.float32)
    per = width // HS
    power = jnp.zeros((batch, 1), jnp.float32)
    for q in range(per):
        cut = slice(q * HS, (q + 1) * HS)
        stream = rows32[pl.ds(NH + half * per + q, batch, stride=rows), :]
        resid = stream + acc[:, cut].astype(jnp.bfloat16).astype(jnp.float32)
        resid_out[:, cut] = resid
        power = power + jnp.sum(resid * resid, axis=-1, keepdims=True)
        scaled = resid * gain[pl.ds(place * per + q, 1), :]
        out[:, cut] = scaled.astype(jnp.bfloat16)
    lanes = lane_iota((batch, HS))
    high, mid, low = split_three(jnp.broadcast_to(power, (batch, HS)))
    zero = jnp.zeros((batch, HS), jnp.float32)
    packed = jnp.where(lanes == 0, high.astype(jnp.float32), zero)
    packed = jnp.where(lanes == 1, mid.astype(jnp.float32), packed)
    packed = jnp.where(lanes == 2, low.astype(jnp.float32), packed)
    out[:, width : width + HS] = packed.astype(jnp.bfloat16)
    tri = (lane_iota((batch, batch)) < row_iota((batch, batch))).astype(jnp.bfloat16)
    onehot = jnp.zeros((batch, HS), jnp.float32)
    picked = jnp.zeros((batch, HS), jnp.float32)
    for expert in range(RESIDENT):
        w = rows32[pl.ds(NH + 2 * per + expert, batch, stride=rows), :]
        named = w > 0.0
        rank = jnp.dot(tri, named.astype(jnp.bfloat16), preferred_element_type=jnp.float32)
        slot = lanes.astype(jnp.float32)
        for turn, low_edge in enumerate((expert * 16 + expert * slots % 8, 32 + expert * slots)):
            inside = (lanes >= low_edge) & (lanes < low_edge + slots)
            hit = inside & named & (rank + float(low_edge) == slot)
            onehot = jnp.where(hit, 1.0, onehot)
            if turn == 0:
                picked = jnp.where(hit, w, picked)
    slot_out[...] = onehot
    pick_out[...] = picked


def merged(left, right):
    return jnp.concatenate([left[:8], left[8:] + right[:8], right[8:]], axis=0)


class UpBlocks:
    def __init__(self, up, ring, sems, side):
        self.up, self.ring, self.sems, self.side = up, ring, sems, side
        self.depth, self.rows, self.narrow = ring.shape
        self.pieces = up.shape[1] // self.rows
        self.total = 4 * RESIDENT * self.pieces
        for k in range(self.depth):
            self.copy(k).start()

    def columns(self, z, side):
        return pl.ds(pl.multiple_of((2 * z + side) * self.narrow, HS), self.narrow)

    def copy(self, k):
        slot = k % self.depth
        block, piece = k // self.pieces, k % self.pieces
        source = self.up.at[
            block % RESIDENT,
            piece * self.rows : (piece + 1) * self.rows,
            self.columns(block // RESIDENT, self.side),
        ]
        return pltpu.make_async_copy(source, self.ring.at[slot], self.sems.at[slot])

    def times(self, lhs, z, expert):
        result = None
        for piece in range(self.pieces):
            k = (z * RESIDENT + expert) * self.pieces + piece
            self.copy(k).wait()
            cut = slice(piece * self.rows, (piece + 1) * self.rows)
            term = jnp.dot(lhs[expert, :, cut], self.ring[k % self.depth], preferred_element_type=jnp.float32)
            result = term if result is None else result + term
            if k + self.depth < self.total:
                self.copy(k + self.depth).start()
        return result


def stacked(work, gate, up, half):
    work[0:half, :] = gate[:half]
    work[half : 2 * half, :] = up[:half]


def both_sides(side, function):
    for fixed in range(2):
        pl.when(side == fixed)(functools.partial(function, fixed))


def side_sums(blocks, lhs, gate, z, side, slots, work):
    columns = slice((2 * z + side) * blocks.narrow, (2 * z + side + 1) * blocks.narrow)
    gates = [
        jnp.dot(lhs[expert], gate[expert, :, columns], preferred_element_type=jnp.float32) for expert in range(RESIDENT)
    ]
    ups = [blocks.times(lhs, z, expert) for expert in range(RESIDENT)]
    stacked(work, merged(*gates), merged(*ups), RESIDENT * slots)


def far_kernel(mine, other, onehot, gate, up, out, lhs_out, place_out, tail_out, ring, sems, work, *, slots):
    batch = mine.shape[0]
    place = lax.axis_index("gx")
    side = place // 2 % 2
    blocks = UpBlocks(up, ring, sems, 1 - side)
    lines = 2 * RESIDENT * slots
    width = mine.shape[1] - HS
    first = place % 2 == 0
    own = mine[:, :width].astype(jnp.float32)
    far = other[:, :width].astype(jnp.float32)
    left = jnp.where(first, own, far).astype(jnp.bfloat16)
    right = jnp.where(first, far, own).astype(jnp.bfloat16)
    hot = onehot[...].astype(jnp.bfloat16)
    over = (((0,), (0,)), ((), ()))
    for at, piece in ((0, left), (width, right)):
        spread = lax.dot_general(hot[:, : RESIDENT * 16], piece, over, preferred_element_type=jnp.float32)
        for expert in range(RESIDENT):
            lhs_out[expert, :, at : at + width] = spread[expert * 16 : (expert + 1) * 16].astype(jnp.bfloat16)
    power = mine[:, width:].astype(jnp.float32) + other[:, width:].astype(jnp.float32)
    power = jnp.sum(power, axis=-1, keepdims=True)
    eye = lane_iota((batch, HS)) == row_iota((batch, HS))
    line = jnp.sum(jnp.where(eye, power, 0.0), axis=0, keepdims=True)
    high, mid, low = split_three(line)
    rows = row_iota((8, HS))
    tail = jnp.where(rows == 0, high.astype(jnp.float32), 0.0)
    tail = jnp.where(rows == 1, mid.astype(jnp.float32), tail)
    tail = jnp.where(rows == 2, low.astype(jnp.float32), tail)
    tail_out[...] = tail
    hot_rows = hot[:, 32 : 32 + place_out.shape[0]]
    place_out[...] = lax.dot_general(hot_rows, eye.astype(jnp.bfloat16), over, preferred_element_type=jnp.float32)

    def run(fixed):
        for z in range(out.shape[0]):
            out[z, out.shape[1] - 8 :, :] = tail.astype(jnp.bfloat16)
            side_sums(blocks, lhs_out, gate, z, fixed, slots, work)
            for q in range(blocks.narrow // HS):
                value = work[:, q * HS : (q + 1) * HS]
                out[z, q * lines : (q + 1) * lines, :] = value.astype(jnp.bfloat16)

    both_sides(1 - side, run)


def near_kernel(lhs, tail, gate, up, out, ring, sems, work, *, slots):
    side = lax.axis_index("gx") // 2 % 2
    blocks = UpBlocks(up, ring, sems, side)
    lines = 2 * RESIDENT * slots

    def run(fixed):
        for z in range(out.shape[0]):
            out[z, out.shape[1] - 8 :, :] = tail[...]
            side_sums(blocks, lhs, gate, z, fixed, slots, work)
            for q in range(blocks.narrow // HS):
                out[z, q * lines : (q + 1) * lines, :] = work[:, q * HS : (q + 1) * HS]

    both_sides(side, run)


def pair_kernel(near_sums, got, keep, *sends):
    z = lax.axis_index("gx") // 4
    keep[...] = near_sums[z] + got[z].astype(jnp.float32)
    for d, send in enumerate(sends, 1):
        send[...] = (near_sums[z ^ d] + got[z ^ d].astype(jnp.float32)).astype(jnp.bfloat16)


def gated_kernel(keep, first, second, third, place, out, work, packed, *, slots, width):
    lines = 2 * RESIDENT * slots
    blocks = out.shape[0]
    per = (keep.shape[0] - 8) // lines
    total = keep[...]
    for got in (first, second, third):
        total = total + got[...].astype(jnp.float32)
    work[...] = total
    line = jnp.sum(work[per * lines : per * lines + 8, :], axis=0, keepdims=True)
    inverse = lax.rsqrt(line / width + 1e-05)
    factor = jnp.sum(place[...] * inverse, axis=-1, keepdims=True)
    half = RESIDENT * slots
    scale = factor[:half, :]
    packed[packed.shape[0] - 8 :, :] = jnp.zeros((8, HS), jnp.float32)
    for q in range(per):
        gate = work[q * lines : q * lines + half, :] * scale
        up = work[q * lines + half : (q + 1) * lines, :] * scale
        packed[q * half : (q + 1) * half, :] = gate / (1.0 + jnp.exp(-gate)) * up
    hidden = packed[...].astype(jnp.bfloat16)
    for block in range(blocks):
        out[block] = hidden


def down_kernel(hidden, down, picked, resid, out, spread, rows32, lhs, acc, *, slots):
    blocks = hidden.shape[0]
    half = lax.axis_index("gx") % 2
    each = RESIDENT * slots
    per = lhs.shape[2] // blocks // HS
    for block in range(blocks):
        rows32[block] = hidden[block].astype(jnp.float32)
        for q in range(per):
            at = (block * per + q) * HS
            for expert in range(RESIDENT):
                start = q * each + expert * slots // 8 * 8
                lhs[expert, :, at : at + HS] = rows32[block, start : start + 16, :].astype(jnp.bfloat16)
    tile = acc.shape[1] // 2

    def columns(k, carry):
        cut = pl.ds(pl.multiple_of(k * tile, tile), tile)
        for expert in range(RESIDENT):
            acc[expert * 16 : (expert + 1) * 16, cut] = jnp.dot(
                lhs[expert], down[expert, :, cut], preferred_element_type=jnp.float32
            )
        return carry

    lax.fori_loop(0, 2, columns, 0)
    weight = picked[...].astype(jnp.bfloat16)[:, : RESIDENT * 16]
    result = None
    for part in split_three(acc[...]):
        term = jnp.dot(weight, part, preferred_element_type=jnp.float32)
        result = term if result is None else result + term
    own = resid[...]
    none = jnp.zeros_like(own)
    width = own.shape[1]
    result = result + jnp.concatenate(
        [jnp.where(half == 0, own, none), jnp.where(half == 0, none, own)], axis=1
    )
    tiles = result.shape[1] // HS
    for q in range(tiles):
        for h in range(2):
            spread[pl.ds(h * tiles + q, blocks, stride=2 * tiles), :] = result[
                h * blocks : (h + 1) * blocks, q * HS : (q + 1) * HS
            ]
    out[...] = spread[...].reshape(out.shape).astype(jnp.bfloat16)


def finish_kernel(got, out):
    blocks = got.shape[0] // 2
    per = got.shape[1]
    for block in range(blocks):
        total = got[2 * block].astype(jnp.float32) + got[2 * block + 1].astype(jnp.float32)
        for q in range(per):
            at = (block * per + q) * HS
            out[0:1, at : at + HS] = total[q : q + 1, :].astype(jnp.bfloat16)


def fast_on_device(
    stream_in,
    query,
    key_new,
    value_new,
    key_cache,
    value_cache,
    lengths,
    route_ids,
    route_scores,
    out_weight,
    norm_gain,
    gate_weight,
    up_weight,
    down_weight,
):
    width = stream_in.shape[1]
    members = lax.axis_size("gx")
    batch = members
    own_width = width // members
    block_width = width // MSPLIT
    hidden_cols = gate_weight.shape[2]
    slots = 5 * batch // 8
    lines = 2 * RESIDENT * slots
    bf16, f32 = jnp.bfloat16, jnp.float32
    chips = [[2 * chip + core for chip in range(MSPLIT)] for core in range(2)]
    swap = [(i, i ^ 1) for i in range(members)]
    V = pltpu.VMEM

    def near(value):
        return pltpu.with_memory_space_constraint(value, V)

    rows = NH + block_width // HS + 8

    def exchange(value, groups):
        return lax.all_to_all(
            value, "gx", split_axis=0, concat_axis=0, tiled=True, axis_index_groups=groups
        )

    loaded = (route_ids, route_scores, query, key_new, value_new, stream_in, key_cache, value_cache)
    (sent,) = one_block(
        attend_kernel,
        [((MSPLIT, rows, HS), bf16)],
        [lengths] + [pltpu.with_memory_space_constraint(value, pltpu.HBM) for value in loaded],
        [pltpu.SMEM] + [pltpu.HBM] * len(loaded),
        "attend",
        scratch=[(pltpu.SMEM if i < 2 else pltpu.VMEM)(value.shape, value.dtype) for i, value in enumerate(loaded)]
        + [pltpu.SemaphoreType.DMA((len(loaded),))]
        + [
            pltpu.VMEM((NH, HS), f32),
            pltpu.VMEM((width // HS, HS), f32),
            pltpu.VMEM((NH, HS), f32),
            pltpu.VMEM((NH, HS), f32),
            pltpu.VMEM((NH, HS), f32),
        ],
        flops=HINT,
    )
    chip_rows = exchange(sent, chips)
    other_rows = lax.ppermute(chip_rows, "gx", swap)
    mine, resid, onehot, picked = one_block(
        functools.partial(project_kernel, slots=slots),
        [((batch, own_width + HS), bf16), ((batch, own_width), f32), ((batch, HS), f32), ((batch, HS), f32)],
        (near(out_weight), chip_rows, other_rows, norm_gain.reshape(width // HS, HS)),
        [V, V, V, V],
        "project",
        scratch=[
            pltpu.VMEM((batch * rows, HS), f32),
            pltpu.VMEM((batch, width), bf16),
            pltpu.VMEM((batch, own_width), f32),
        ],
    )
    other = lax.ppermute(mine, "gx", swap)
    narrow = hidden_cols // MSPLIT
    per = narrow // HS
    held = -(-RESIDENT * slots // 8) * 8
    chunk = (per * lines + 8, HS)
    flat = (-(-per * RESIDENT * slots // 8) * 8, HS)
    up_hbm = pltpu.with_memory_space_constraint(up_weight, pltpu.HBM)

    def side_scratch(depth):
        return [
            pltpu.VMEM((depth, block_width // 2, narrow), bf16),
            pltpu.SemaphoreType.DMA((depth,)),
            pltpu.VMEM((lines, narrow), f32),
        ]

    far, lhs, place, tail = one_block(
        functools.partial(far_kernel, slots=slots),
        [((4,) + chunk, bf16), ((RESIDENT, 16, block_width), bf16), ((held, HS), f32), ((8, HS), f32)],
        (near(mine), near(other), near(onehot), near(gate_weight), up_hbm),
        [V, V, V, V, pltpu.HBM],
        "far",
        scratch=side_scratch(6),
        grant=7 << 20,
    )
    crossed = lax.ppermute(far, "gx", [(i, i ^ 2) for i in range(members)])
    (near_sums,) = one_block(
        functools.partial(near_kernel, slots=slots),
        [((4,) + chunk, f32)],
        (lhs, tail, near(gate_weight), up_hbm),
        [V, V, V, pltpu.HBM],
        "near",
        scratch=side_scratch(6),
        grant=7 << 20,
    )
    keep, *sends = one_block(
        pair_kernel, [(chunk, f32)] + [(chunk, bf16)] * 3, (near_sums, crossed), [V, V], "pair", flops=HINT // 5
    )
    got = [lax.ppermute(sends[d - 1], "gx", [(i, i ^ 4 * d) for i in range(members)]) for d in (1, 2, 3)]
    (hidden,) = one_block(
        functools.partial(gated_kernel, slots=slots, width=width),
        [((MSPLIT,) + flat, bf16)],
        (keep, *got, place),
        [V] * 5,
        "gated",
        scratch=[pltpu.VMEM(chunk, f32), pltpu.VMEM(flat, f32)],
        flops=HINT // 5,
    )
    hidden_all = exchange(hidden, chips)
    (partial_out,) = one_block(
        functools.partial(down_kernel, slots=slots),
        [((members, block_width // HS, HS), bf16)],
        (hidden_all, near(down_weight), picked, resid),
        [V, V, V, V],
        "down",
        scratch=[
            pltpu.VMEM((members * block_width // HS, HS), f32),
            pltpu.VMEM((MSPLIT,) + flat, f32),
            pltpu.VMEM((RESIDENT, 16, hidden_cols), bf16),
            pltpu.VMEM((RESIDENT * 16, block_width), f32),
        ],
    )
    last = exchange(partial_out, None)
    (out,) = one_block(finish_kernel, [((1, width), bf16)], (last,), [V], "finish")
    return out


def fits(shapes, members):
    width = shapes[0][1]
    hidden_cols = shapes[11][2]
    return (
        members == 2 * MSPLIT
        and shapes[0][0] == 1
        and shapes[4][1] == HS
        and width == NH * HS
        and width % (members * HS) == 0
        and hidden_cols % (MSPLIT * HS) == 0
        and (5 * members) % 8 == 0
        and 8 <= 5 * members // 8 <= 14
        and RESIDENT == 2
    )


def on_device(*args):
    if fits([arg.shape for arg in args], lax.axis_size("gx")):
        return fast_on_device(*args)
    return plain_on_device(*args)


def solution(mesh):
    return jax.shard_map(
        on_device,
        mesh=mesh,
        in_specs=(
            P(("groups", "gx"), None),
            P(("groups", "gx"), None),
            P(("groups", "gx"), None),
            P(("groups", "gx"), None),
            P(("groups", "gx"), None, None),
            P(("groups", "gx"), None, None),
            P(("groups", "gx")),
            P(("groups", "gx"), None),
            P(("groups", "gx"), None),
            P(None, "gx"),
            P(),
            P(None, "gx", None),
            P(None, "gx", None),
            P(None, "gx", None),
        ),
        out_specs=P(("groups", "gx"), None),
        check_vma=False,
    )
```

```python
import functools

import jax
import jax.numpy as jnp
from jax import lax
from jax.experimental import pallas as pl
from jax.experimental.pallas import tpu as pltpu
from jax.sharding import PartitionSpec as P

NH = 64
KVH = 8
HS = 128
RESIDENT = 2
MSPLIT = 8
HINT = 100_000_000_000


def partner(value, axis, distance):
    return lax.ppermute(value, axis, [(i, i ^ 1 << distance) for i in range(lax.axis_size(axis))])


def attend_local(query, key_new, value_new, key_cache, value_cache, lengths):
    seqs = query.shape[0]
    slots = key_cache.shape[1]
    group = NH // KVH
    scale = HS ** (-0.5)
    q_four = query.reshape(seqs, KVH, group, HS)
    k_all = key_cache.reshape(seqs, slots, KVH, HS)
    v_all = value_cache.reshape(seqs, slots, KVH, HS)
    k_own = key_new.reshape(seqs, KVH, HS)
    v_own = value_new.reshape(seqs, KVH, HS)
    scores = (
        jnp.einsum("skgd,sckd->skgc", q_four, k_all, preferred_element_type=jnp.float32) * scale
    )
    live = jnp.arange(slots, dtype=jnp.int32)[None, :] < lengths[:, None]
    scores = jnp.where(live[:, None, None, :], scores, -1e30)
    own = jnp.einsum("skgd,skd->skg", q_four, k_own, preferred_element_type=jnp.float32) * scale
    top = jnp.maximum(jnp.max(scores, axis=-1), own)
    e_cache = jnp.exp(scores - top[..., None])
    e_own = jnp.exp(own - top)
    total = jnp.sum(e_cache, axis=-1) + e_own
    p_cache = (e_cache / total[..., None]).astype(jnp.bfloat16)
    p_own = (e_own / total).astype(jnp.bfloat16)
    mixed = jnp.einsum("skgc,sckd->skgd", p_cache, v_all, preferred_element_type=jnp.float32)
    mixed = mixed + p_own.astype(jnp.float32)[..., None] * v_own.astype(jnp.float32)[:, :, None, :]
    return mixed.reshape(seqs, NH * HS).astype(jnp.bfloat16)


def gated(parts):
    return (jax.nn.silu(parts[..., 0, :]) * parts[..., 1, :]).astype(jnp.bfloat16)


def plain_on_device(
    stream_in,
    query,
    key_new,
    value_new,
    key_cache,
    value_cache,
    lengths,
    route_ids,
    route_scores,
    out_weight,
    norm_gain,
    gate_weight,
    up_weight,
    down_weight,
):
    seqs = stream_in.shape[0]
    width = stream_in.shape[1]
    members = lax.axis_size("gx")
    batch = seqs * members
    hsplit = members // MSPLIT
    low_bits = hsplit.bit_length() - 1
    model_bits = MSPLIT.bit_length() - 1
    place = lax.axis_index("gx")
    model_block = place // hsplit
    block_width = width // MSPLIT
    hidden_cols = gate_weight.shape[2]
    narrow = hidden_cols // MSPLIT
    attn = attend_local(query, key_new, value_new, key_cache, value_cache, lengths)
    proj_cols = jnp.dot(
        lax.all_gather(attn, "gx", axis=0, tiled=True),
        out_weight,
        preferred_element_type=jnp.float32,
    ).astype(jnp.bfloat16)
    proj = lax.all_to_all(proj_cols, "gx", split_axis=0, concat_axis=1, tiled=True)
    resid = stream_in.astype(jnp.float32) + proj.astype(jnp.float32)
    power = jnp.mean(resid * resid, axis=-1, keepdims=True)
    normed = (resid * lax.rsqrt(power + 1e-05) * norm_gain).astype(jnp.bfloat16)
    probs = jax.nn.softmax(route_scores, axis=-1)
    columns = []
    for expert in range(RESIDENT):
        columns.append(jnp.sum(jnp.where(route_ids == expert, probs, 0.0), axis=-1))
    weight = jnp.stack(columns, axis=-1).astype(jnp.bfloat16)
    normed_all, weight_all = (
        lax.all_gather(normed, "gx", axis=0, tiled=True),
        lax.all_gather(weight, "gx", axis=0, tiled=True),
    )
    rows_in = lax.dynamic_slice_in_dim(normed_all, model_block * block_width, block_width, 1)
    gate_view = gate_weight.reshape(RESIDENT, block_width, MSPLIT, narrow)
    up_view = up_weight.reshape(RESIDENT, block_width, MSPLIT, narrow)
    gate_part = jnp.einsum("bd,rdpc->bprc", rows_in, gate_view, preferred_element_type=jnp.float32)
    up_part = jnp.einsum("bd,rdpc->bprc", rows_in, up_view, preferred_element_type=jnp.float32)
    parts = jnp.stack([gate_part, up_part], axis=3)
    for bit in range(model_bits):
        parts = parts + partner(parts.astype(jnp.bfloat16), "gx", low_bits + bit).astype(
            parts.dtype
        )
    hidden = gated(parts)
    down_view = down_weight.reshape(RESIDENT, MSPLIT, narrow, block_width)
    scales = weight_all.astype(jnp.float32)
    result = jnp.zeros((batch, block_width), jnp.float32)
    for expert in range(RESIDENT):
        term = jnp.einsum(
            "bpc,pcn->bn",
            hidden[:, :, expert],
            down_view[expert],
            preferred_element_type=jnp.float32,
        )
        result = result + scales[:, expert][:, None] * term
    partial_out = result.reshape(members, seqs, block_width)
    got = lax.all_to_all(
        partial_out.astype(jnp.bfloat16), "gx", split_axis=0, concat_axis=0, tiled=True
    ).astype(partial_out.dtype)
    got = jnp.sum(got.reshape(MSPLIT, hsplit, seqs, block_width), axis=1)
    ffn = got.transpose(1, 0, 2).reshape(seqs, width)
    return (resid + ffn).astype(jnp.bfloat16)


def lane_iota(shape):
    return lax.broadcasted_iota(jnp.int32, shape, len(shape) - 1)


def row_iota(shape):
    return lax.broadcasted_iota(jnp.int32, shape, 0)


def split_three(value):
    high = value.astype(jnp.bfloat16)
    rest = value - high.astype(jnp.float32)
    mid = rest.astype(jnp.bfloat16)
    low = (rest - mid.astype(jnp.float32)).astype(jnp.bfloat16)
    return high, mid, low


def one_block(kernel, outs, args, spaces, name, scratch=(), flops=0, grant=3 << 20):
    return pl.pallas_call(
        kernel,
        out_shape=[jax.ShapeDtypeStruct(shape, dtype) for shape, dtype in outs],
        in_specs=[pl.BlockSpec(memory_space=space) for space in spaces],
        out_specs=[pl.BlockSpec(memory_space=pltpu.VMEM) for _ in outs],
        scratch_shapes=list(scratch),
        cost_estimate=pl.CostEstimate(flops=flops, transcendentals=0, bytes_accessed=1 << 20),
        compiler_params=pltpu.CompilerParams(vmem_limit_bytes=grant),
        name=name,
    )(*args)


def attend_kernel(*refs):
    lengths, sources, out, places, sems, work = refs[0], refs[1:9], refs[9], refs[10:18], refs[18], refs[19:]
    copies = [
        pltpu.make_async_copy(source, place, sems.at[i])
        for i, (source, place) in enumerate(zip(sources, places))
    ]
    for copy in copies:
        copy.start()
    for copy in copies:
        copy.wait()
    ids, scores_in, query, key_new, value_new, stream, keys, values = places
    q_rows, s_rows, own_k, own_v, s_acc = work
    blocks, rows = out.shape[0], out.shape[1]
    group = NH // KVH
    for head in range(NH):
        q_rows[head : head + 1, :] = query[0:1, head * HS : (head + 1) * HS].astype(jnp.float32)
    for tile in range(s_rows.shape[0]):
        s_rows[tile : tile + 1, :] = stream[0:1, tile * HS : (tile + 1) * HS].astype(jnp.float32)
    for g in range(KVH):
        cut = slice(g * HS, (g + 1) * HS)
        here = slice(g * group, (g + 1) * group)
        own_k[here, :] = jnp.broadcast_to(key_new[0:1, cut].astype(jnp.float32), (group, HS))
        own_v[here, :] = jnp.broadcast_to(value_new[0:1, cut].astype(jnp.float32), (group, HS))
        s_acc[here, :] = lax.dot_general(
            q_rows[here, :].astype(jnp.bfloat16),
            keys[0, :, cut],
            (((1,), (1,)), ((), ())),
            preferred_element_type=jnp.float32,
        )
    scale = HS ** (-0.5)
    scores = s_acc[...] * scale
    scores = jnp.where(lane_iota(scores.shape) < lengths[0], scores, -1e30)
    own = jnp.sum(q_rows[...] * own_k[...], axis=-1, keepdims=True) * scale
    top = jnp.maximum(jnp.max(scores, axis=-1, keepdims=True), own)
    e_cache = jnp.exp(scores - top)
    e_own = jnp.exp(own - top)
    total = jnp.sum(e_cache, axis=-1, keepdims=True) + e_own
    p_cache = e_cache / total
    p_own = (e_own / total).astype(jnp.bfloat16).astype(jnp.float32)
    s_acc[...] = p_cache
    for g in range(KVH):
        cut = slice(g * HS, (g + 1) * HS)
        here = slice(g * group, (g + 1) * group)
        mixed = jnp.dot(
            s_acc[here, :].astype(jnp.bfloat16), values[0, :, cut], preferred_element_type=jnp.float32
        )
        q_rows[here, :] = mixed + p_own[here, :] * own_v[here, :]
    attn = q_rows[...].astype(jnp.bfloat16)
    first = jnp.full((8, HS), scores_in[0, 0])
    second = jnp.full((8, HS), scores_in[0, 1])
    peak = jnp.maximum(first, second)
    e_first = jnp.exp(first - peak)
    e_second = jnp.exp(second - peak)
    both = e_first + e_second
    tail = jnp.zeros((8, HS), jnp.float32)
    for expert in range(RESIDENT):
        w = jnp.where(ids[0, 0] == expert, e_first / both, 0.0)
        w = w + jnp.where(ids[0, 1] == expert, e_second / both, 0.0)
        tail = jnp.where(row_iota(tail.shape) == expert, w, tail)
    tail = tail.astype(jnp.bfloat16)
    per = s_rows.shape[0] // blocks
    for block in range(blocks):
        out[block, 0:NH, :] = attn
        out[block, NH : NH + per, :] = s_rows[block * per : (block + 1) * per, :].astype(jnp.bfloat16)
        out[block, NH + per : rows, :] = tail


def project_kernel(weight, here, there, gain, out, resid_out, slot_out, pick_out, rows32, lhs, acc, *, slots):
    batch, width = acc.shape
    chips, rows = here.shape[:2]
    place = lax.axis_index("gx")
    half = place % 2
    for source, core in ((here, half), (there, 1 - half)):
        first = pl.multiple_of(core * (chips * rows), 8)
        rows32[pl.ds(first, chips * rows), :] = source[...].reshape(chips * rows, HS).astype(jnp.float32)
    for head in range(NH):
        lhs[:, head * HS : (head + 1) * HS] = rows32[pl.ds(head, batch, stride=rows), :].astype(jnp.bfloat16)
    acc[...] = jnp.dot(lhs[...], weight[...], preferred_element_type=jnp.float32)
    per = width // HS
    power = jnp.zeros((batch, 1), jnp.float32)
    for q in range(per):
        cut = slice(q * HS, (q + 1) * HS)
        stream = rows32[pl.ds(NH + half * per + q, batch, stride=rows), :]
        resid = stream + acc[:, cut].astype(jnp.bfloat16).astype(jnp.float32)
        resid_out[:, cut] = resid
        power = power + jnp.sum(resid * resid, axis=-1, keepdims=True)
        scaled = resid * gain[pl.ds(place * per + q, 1), :]
        out[:, cut] = scaled.astype(jnp.bfloat16)
    lanes = lane_iota((batch, HS))
    high, mid, low = split_three(jnp.broadcast_to(power, (batch, HS)))
    zero = jnp.zeros((batch, HS), jnp.float32)
    packed = jnp.where(lanes == 0, high.astype(jnp.float32), zero)
    packed = jnp.where(lanes == 1, mid.astype(jnp.float32), packed)
    packed = jnp.where(lanes == 2, low.astype(jnp.float32), packed)
    out[:, width : width + HS] = packed.astype(jnp.bfloat16)
    tri = (lane_iota((batch, batch)) < row_iota((batch, batch))).astype(jnp.bfloat16)
    onehot = jnp.zeros((batch, HS), jnp.float32)
    picked = jnp.zeros((batch, HS), jnp.float32)
    for expert in range(RESIDENT):
        w = rows32[pl.ds(NH + 2 * per + expert, batch, stride=rows), :]
        named = w > 0.0
        rank = jnp.dot(tri, named.astype(jnp.bfloat16), preferred_element_type=jnp.float32)
        slot = lanes.astype(jnp.float32)
        for turn, low_edge in enumerate((expert * 16 + expert * slots % 8, 32 + expert * slots)):
            inside = (lanes >= low_edge) & (lanes < low_edge + slots)
            hit = inside & named & (rank + float(low_edge) == slot)
            onehot = jnp.where(hit, 1.0, onehot)
            if turn == 0:
                picked = jnp.where(hit, w, picked)
    slot_out[...] = onehot
    pick_out[...] = picked


def merged(left, right):
    return jnp.concatenate([left[:8], left[8:] + right[:8], right[8:]], axis=0)


class UpBlocks:
    def __init__(self, up, ring, sems, side):
        self.up, self.ring, self.sems, self.side = up, ring, sems, side
        self.depth, self.rows, self.narrow = ring.shape
        self.pieces = up.shape[1] // self.rows
        self.total = 4 * RESIDENT * self.pieces
        for k in range(self.depth):
            self.copy(k).start()

    def columns(self, z, side):
        return pl.ds(pl.multiple_of((2 * z + side) * self.narrow, HS), self.narrow)

    def copy(self, k):
        slot = k % self.depth
        block, piece = k // self.pieces, k % self.pieces
        source = self.up.at[
            block % RESIDENT,
            piece * self.rows : (piece + 1) * self.rows,
            self.columns(block // RESIDENT, self.side),
        ]
        return pltpu.make_async_copy(source, self.ring.at[slot], self.sems.at[slot])

    def times(self, lhs, z, expert):
        result = None
        for piece in range(self.pieces):
            k = (z * RESIDENT + expert) * self.pieces + piece
            self.copy(k).wait()
            cut = slice(piece * self.rows, (piece + 1) * self.rows)
            term = jnp.dot(lhs[expert, :, cut], self.ring[k % self.depth], preferred_element_type=jnp.float32)
            result = term if result is None else result + term
            if k + self.depth < self.total:
                self.copy(k + self.depth).start()
        return result


def stacked(work, gate, up, half):
    work[0:half, :] = gate[:half]
    work[half : 2 * half, :] = up[:half]


def both_sides(side, function):
    for fixed in range(2):
        pl.when(side == fixed)(functools.partial(function, fixed))


def side_sums(blocks, lhs, gate, z, side, slots, work):
    columns = slice((2 * z + side) * blocks.narrow, (2 * z + side + 1) * blocks.narrow)
    gates = [
        jnp.dot(lhs[expert], gate[expert, :, columns], preferred_element_type=jnp.float32) for expert in range(RESIDENT)
    ]
    ups = [blocks.times(lhs, z, expert) for expert in range(RESIDENT)]
    stacked(work, merged(*gates), merged(*ups), RESIDENT * slots)


def far_kernel(mine, other, onehot, gate, up, out, lhs_out, place_out, tail_out, ring, sems, work, *, slots):
    batch = mine.shape[0]
    place = lax.axis_index("gx")
    side = place // 2 % 2
    blocks = UpBlocks(up, ring, sems, 1 - side)
    lines = 2 * RESIDENT * slots
    width = mine.shape[1] - HS
    first = place % 2 == 0
    own = mine[:, :width].astype(jnp.float32)
    far = other[:, :width].astype(jnp.float32)
    left = jnp.where(first, own, far).astype(jnp.bfloat16)
    right = jnp.where(first, far, own).astype(jnp.bfloat16)
    hot = onehot[...].astype(jnp.bfloat16)
    over = (((0,), (0,)), ((), ()))
    for at, piece in ((0, left), (width, right)):
        spread = lax.dot_general(hot[:, : RESIDENT * 16], piece, over, preferred_element_type=jnp.float32)
        for expert in range(RESIDENT):
            lhs_out[expert, :, at : at + width] = spread[expert * 16 : (expert + 1) * 16].astype(jnp.bfloat16)
    power = mine[:, width:].astype(jnp.float32) + other[:, width:].astype(jnp.float32)
    power = jnp.sum(power, axis=-1, keepdims=True)
    eye = lane_iota((batch, HS)) == row_iota((batch, HS))
    line = jnp.sum(jnp.where(eye, power, 0.0), axis=0, keepdims=True)
    high, mid, low = split_three(line)
    rows = row_iota((8, HS))
    tail = jnp.where(rows == 0, high.astype(jnp.float32), 0.0)
    tail = jnp.where(rows == 1, mid.astype(jnp.float32), tail)
    tail = jnp.where(rows == 2, low.astype(jnp.float32), tail)
    tail_out[...] = tail
    hot_rows = hot[:, 32 : 32 + place_out.shape[0]]
    place_out[...] = lax.dot_general(hot_rows, eye.astype(jnp.bfloat16), over, preferred_element_type=jnp.float32)

    def run(fixed):
        for z in range(out.shape[0]):
            out[z, out.shape[1] - 8 :, :] = tail.astype(jnp.bfloat16)
            side_sums(blocks, lhs_out, gate, z, fixed, slots, work)
            for q in range(blocks.narrow // HS):
                value = work[:, q * HS : (q + 1) * HS]
                out[z, q * lines : (q + 1) * lines, :] = value.astype(jnp.bfloat16)

    both_sides(1 - side, run)


def near_kernel(lhs, tail, gate, up, out, ring, sems, work, *, slots):
    side = lax.axis_index("gx") // 2 % 2
    blocks = UpBlocks(up, ring, sems, side)
    lines = 2 * RESIDENT * slots

    def run(fixed):
        for z in range(out.shape[0]):
            out[z, out.shape[1] - 8 :, :] = tail[...]
            side_sums(blocks, lhs, gate, z, fixed, slots, work)
            for q in range(blocks.narrow // HS):
                out[z, q * lines : (q + 1) * lines, :] = work[:, q * HS : (q + 1) * HS]

    both_sides(side, run)


def pair_kernel(near_sums, got, keep, *sends):
    z = lax.axis_index("gx") // 4
    keep[...] = near_sums[z] + got[z].astype(jnp.float32)
    for d, send in enumerate(sends, 1):
        send[...] = (near_sums[z ^ d] + got[z ^ d].astype(jnp.float32)).astype(jnp.bfloat16)


def gated_kernel(keep, first, second, third, place, out, work, packed, *, slots, width):
    lines = 2 * RESIDENT * slots
    per = (keep.shape[0] - 8) // lines
    total = keep[...]
    for got in (first, second, third):
        total = total + got[...].astype(jnp.float32)
    work[...] = total
    line = jnp.sum(work[per * lines : per * lines + 8, :], axis=0, keepdims=True)
    inverse = lax.rsqrt(line / width + 1e-05)
    factor = jnp.sum(place[...] * inverse, axis=-1, keepdims=True)
    half = RESIDENT * slots
    scale = factor[:half, :]
    packed[packed.shape[0] - 8 :, :] = jnp.zeros((8, HS), jnp.float32)
    for q in range(per):
        gate = work[q * lines : q * lines + half, :] * scale
        up = work[q * lines + half : (q + 1) * lines, :] * scale
        packed[q * half : (q + 1) * half, :] = gate / (1.0 + jnp.exp(-gate)) * up
    out[...] = packed[...].astype(jnp.bfloat16)


def gather_kernel(own, first, second, third, out):
    for d, value in enumerate((own, first, second, third)):
        out[d] = value[...]


def down_side(hidden, down, side, rows32, lhs, acc, slots):
    own = lax.axis_index("gx") // 4
    each = RESIDENT * slots
    narrow = lhs.shape[3]
    for z in range(4):
        rows32[z] = hidden[z ^ own].astype(jnp.float32)
        for q in range(narrow // HS):
            for expert in range(RESIDENT):
                start = q * each + expert * slots // 8 * 8
                piece = rows32[z, start : start + 16, :]
                lhs[z, expert, :, q * HS : (q + 1) * HS] = piece.astype(jnp.bfloat16)

    def run(fixed):
        for expert in range(RESIDENT):
            total = None
            for z in range(4):
                cut = slice((2 * z + fixed) * narrow, (2 * z + fixed + 1) * narrow)
                term = jnp.dot(lhs[z, expert], down[expert, cut, :], preferred_element_type=jnp.float32)
                total = term if total is None else total + term
            acc[expert * 16 : (expert + 1) * 16, :] = total

    both_sides(side, run)


def down_near_kernel(hidden, down, acc, rows32, lhs, *, slots):
    down_side(hidden, down, lax.axis_index("gx") // 2 % 2, rows32, lhs, acc, slots)


def down_far_kernel(hidden, down, near_acc, picked, resid, out, spread, rows32, lhs, acc, *, slots):
    down_side(hidden, down, 1 - lax.axis_index("gx") // 2 % 2, rows32, lhs, acc, slots)
    half = lax.axis_index("gx") % 2
    blocks = 8
    acc[...] = acc[...] + near_acc[...]
    weight = picked[...].astype(jnp.bfloat16)[:, : RESIDENT * 16]
    result = None
    for part in split_three(acc[...]):
        term = jnp.dot(weight, part, preferred_element_type=jnp.float32)
        result = term if result is None else result + term
    own = resid[...]
    none = jnp.zeros_like(own)
    width = own.shape[1]
    result = result + jnp.concatenate(
        [jnp.where(half == 0, own, none), jnp.where(half == 0, none, own)], axis=1
    )
    tiles = result.shape[1] // HS
    for q in range(tiles):
        for h in range(2):
            spread[pl.ds(h * tiles + q, blocks, stride=2 * tiles), :] = result[
                h * blocks : (h + 1) * blocks, q * HS : (q + 1) * HS
            ]
    out[...] = spread[...].reshape(out.shape).astype(jnp.bfloat16)


def finish_kernel(got, out):
    blocks = got.shape[0] // 2
    per = got.shape[1]
    for block in range(blocks):
        total = got[2 * block].astype(jnp.float32) + got[2 * block + 1].astype(jnp.float32)
        for q in range(per):
            at = (block * per + q) * HS
            out[0:1, at : at + HS] = total[q : q + 1, :].astype(jnp.bfloat16)


HG = 0


def fast_on_device(
    stream_in,
    query,
    key_new,
    value_new,
    key_cache,
    value_cache,
    lengths,
    route_ids,
    route_scores,
    out_weight,
    norm_gain,
    gate_weight,
    up_weight,
    down_weight,
):
    width = stream_in.shape[1]
    members = lax.axis_size("gx")
    batch = members
    own_width = width // members
    block_width = width // MSPLIT
    hidden_cols = gate_weight.shape[2]
    slots = 5 * batch // 8
    lines = 2 * RESIDENT * slots
    bf16, f32 = jnp.bfloat16, jnp.float32
    chips = [[2 * chip + core for chip in range(MSPLIT)] for core in range(2)]
    swap = [(i, i ^ 1) for i in range(members)]
    V = pltpu.VMEM

    def near(value):
        return pltpu.with_memory_space_constraint(value, V)

    rows = NH + block_width // HS + 8

    def exchange(value, groups):
        return lax.all_to_all(
            value, "gx", split_axis=0, concat_axis=0, tiled=True, axis_index_groups=groups
        )

    loaded = (route_ids, route_scores, query, key_new, value_new, stream_in, key_cache, value_cache)
    (sent,) = one_block(
        attend_kernel,
        [((MSPLIT, rows, HS), bf16)],
        [lengths] + [pltpu.with_memory_space_constraint(value, pltpu.HBM) for value in loaded],
        [pltpu.SMEM] + [pltpu.HBM] * len(loaded),
        "attend",
        scratch=[(pltpu.SMEM if i < 2 else pltpu.VMEM)(value.shape, value.dtype) for i, value in enumerate(loaded)]
        + [pltpu.SemaphoreType.DMA((len(loaded),))]
        + [
            pltpu.VMEM((NH, HS), f32),
            pltpu.VMEM((width // HS, HS), f32),
            pltpu.VMEM((NH, HS), f32),
            pltpu.VMEM((NH, HS), f32),
            pltpu.VMEM((NH, HS), f32),
        ],
        flops=HINT,
    )
    chip_rows = exchange(sent, chips)
    other_rows = lax.ppermute(chip_rows, "gx", swap)
    mine, resid, onehot, picked = one_block(
        functools.partial(project_kernel, slots=slots),
        [((batch, own_width + HS), bf16), ((batch, own_width), f32), ((batch, HS), f32), ((batch, HS), f32)],
        (near(out_weight), chip_rows, other_rows, norm_gain.reshape(width // HS, HS)),
        [V, V, V, V],
        "project",
        scratch=[
            pltpu.VMEM((batch * rows, HS), f32),
            pltpu.VMEM((batch, width), bf16),
            pltpu.VMEM((batch, own_width), f32),
        ],
    )
    other = lax.ppermute(mine, "gx", swap)
    narrow = hidden_cols // MSPLIT
    per = narrow // HS
    held = -(-RESIDENT * slots // 8) * 8
    chunk = (per * lines + 8, HS)
    flat = (-(-per * RESIDENT * slots // 8) * 8, HS)
    up_hbm = pltpu.with_memory_space_constraint(up_weight, pltpu.HBM)

    def side_scratch(depth):
        return [
            pltpu.VMEM((depth, block_width // 2, narrow), bf16),
            pltpu.SemaphoreType.DMA((depth,)),
            pltpu.VMEM((lines, narrow), f32),
        ]

    far, lhs, place, tail = one_block(
        functools.partial(far_kernel, slots=slots),
        [((4,) + chunk, bf16), ((RESIDENT, 16, block_width), bf16), ((held, HS), f32), ((8, HS), f32)],
        (near(mine), near(other), near(onehot), near(gate_weight), up_hbm),
        [V, V, V, V, pltpu.HBM],
        "far",
        scratch=side_scratch(6),
        grant=7 << 20,
    )
    crossed = lax.ppermute(far, "gx", [(i, i ^ 2) for i in range(members)])
    (near_sums,) = one_block(
        functools.partial(near_kernel, slots=slots),
        [((4,) + chunk, f32)],
        (lhs, tail, near(gate_weight), up_hbm),
        [V, V, V, pltpu.HBM],
        "near",
        scratch=side_scratch(6),
        grant=7 << 20,
    )
    keep, *sends = one_block(
        pair_kernel, [(chunk, f32)] + [(chunk, bf16)] * 3, (near_sums, crossed), [V, V], "pair", flops=HINT // 5
    )
    got = [lax.ppermute(sends[d - 1], "gx", [(i, i ^ 4 * d) for i in range(members)]) for d in (1, 2, 3)]
    (hidden,) = one_block(
        functools.partial(gated_kernel, slots=slots, width=width),
        [(flat, bf16)],
        (keep, *got, place),
        [V] * 5,
        "gated",
        scratch=[pltpu.VMEM(chunk, f32), pltpu.VMEM(flat, f32)],
        flops=HINT // 5,
    )
    parts = [lax.ppermute(hidden, "gx", [(i, i ^ 4 * d) for i in range(members)]) for d in (1, 2, 3)]
    (near_hidden,) = one_block(gather_kernel, [((4,) + flat, bf16)], (hidden, *parts), [V] * 4, "gather", flops=HG)
    far_hidden = lax.ppermute(near_hidden, "gx", [(i, i ^ 2) for i in range(members)])
    side_rows = [pltpu.VMEM((4,) + flat, f32), pltpu.VMEM((4, RESIDENT, 16, narrow), bf16)]
    sums = (RESIDENT * 16, block_width)
    (near_acc,) = one_block(
        functools.partial(down_near_kernel, slots=slots),
        [(sums, f32)],
        (near_hidden, near(down_weight)),
        [V, V],
        "down_near",
        scratch=side_rows,
    )
    (partial_out,) = one_block(
        functools.partial(down_far_kernel, slots=slots),
        [((members, block_width // HS, HS), bf16)],
        (far_hidden, near(down_weight), near_acc, picked, resid),
        [V] * 5,
        "down_far",
        scratch=[pltpu.VMEM((members * block_width // HS, HS), f32)] + side_rows + [pltpu.VMEM(sums, f32)],
    )
    last = exchange(partial_out, None)
    (out,) = one_block(finish_kernel, [((1, width), bf16)], (last,), [V], "finish")
    return out


def fits(shapes, members):
    width = shapes[0][1]
    hidden_cols = shapes[11][2]
    return (
        members == 2 * MSPLIT
        and shapes[0][0] == 1
        and shapes[4][1] == HS
        and width == NH * HS
        and width % (members * HS) == 0
        and hidden_cols % (MSPLIT * HS) == 0
        and (5 * members) % 8 == 0
        and 8 <= 5 * members // 8 <= 14
        and RESIDENT == 2
    )


def on_device(*args):
    if fits([arg.shape for arg in args], lax.axis_size("gx")):
        return fast_on_device(*args)
    return plain_on_device(*args)


def solution(mesh):
    return jax.shard_map(
        on_device,
        mesh=mesh,
        in_specs=(
            P(("groups", "gx"), None),
            P(("groups", "gx"), None),
            P(("groups", "gx"), None),
            P(("groups", "gx"), None),
            P(("groups", "gx"), None, None),
            P(("groups", "gx"), None, None),
            P(("groups", "gx")),
            P(("groups", "gx"), None),
            P(("groups", "gx"), None),
            P(None, "gx"),
            P(),
            P(None, "gx", None),
            P(None, "gx", None),
            P(None, "gx", None),
        ),
        out_specs=P(("groups", "gx"), None),
        check_vma=False,
    )
```

```python
import functools

import jax
import jax.numpy as jnp
from jax import lax
from jax.experimental import pallas as pl
from jax.experimental.pallas import tpu as pltpu
from jax.sharding import PartitionSpec as P

NH = 64
KVH = 8
HS = 128
RESIDENT = 2
MSPLIT = 8
HINT = 100_000_000_000


def partner(value, axis, distance):
    return lax.ppermute(value, axis, [(i, i ^ 1 << distance) for i in range(lax.axis_size(axis))])


def attend_local(query, key_new, value_new, key_cache, value_cache, lengths):
    seqs = query.shape[0]
    slots = key_cache.shape[1]
    group = NH // KVH
    scale = HS ** (-0.5)
    q_four = query.reshape(seqs, KVH, group, HS)
    k_all = key_cache.reshape(seqs, slots, KVH, HS)
    v_all = value_cache.reshape(seqs, slots, KVH, HS)
    k_own = key_new.reshape(seqs, KVH, HS)
    v_own = value_new.reshape(seqs, KVH, HS)
    scores = (
        jnp.einsum("skgd,sckd->skgc", q_four, k_all, preferred_element_type=jnp.float32) * scale
    )
    live = jnp.arange(slots, dtype=jnp.int32)[None, :] < lengths[:, None]
    scores = jnp.where(live[:, None, None, :], scores, -1e30)
    own = jnp.einsum("skgd,skd->skg", q_four, k_own, preferred_element_type=jnp.float32) * scale
    top = jnp.maximum(jnp.max(scores, axis=-1), own)
    e_cache = jnp.exp(scores - top[..., None])
    e_own = jnp.exp(own - top)
    total = jnp.sum(e_cache, axis=-1) + e_own
    p_cache = (e_cache / total[..., None]).astype(jnp.bfloat16)
    p_own = (e_own / total).astype(jnp.bfloat16)
    mixed = jnp.einsum("skgc,sckd->skgd", p_cache, v_all, preferred_element_type=jnp.float32)
    mixed = mixed + p_own.astype(jnp.float32)[..., None] * v_own.astype(jnp.float32)[:, :, None, :]
    return mixed.reshape(seqs, NH * HS).astype(jnp.bfloat16)


def gated(parts):
    return (jax.nn.silu(parts[..., 0, :]) * parts[..., 1, :]).astype(jnp.bfloat16)


def plain_on_device(
    stream_in,
    query,
    key_new,
    value_new,
    key_cache,
    value_cache,
    lengths,
    route_ids,
    route_scores,
    out_weight,
    norm_gain,
    gate_weight,
    up_weight,
    down_weight,
):
    seqs = stream_in.shape[0]
    width = stream_in.shape[1]
    members = lax.axis_size("gx")
    batch = seqs * members
    hsplit = members // MSPLIT
    low_bits = hsplit.bit_length() - 1
    model_bits = MSPLIT.bit_length() - 1
    place = lax.axis_index("gx")
    model_block = place // hsplit
    block_width = width // MSPLIT
    hidden_cols = gate_weight.shape[2]
    narrow = hidden_cols // MSPLIT
    attn = attend_local(query, key_new, value_new, key_cache, value_cache, lengths)
    proj_cols = jnp.dot(
        lax.all_gather(attn, "gx", axis=0, tiled=True),
        out_weight,
        preferred_element_type=jnp.float32,
    ).astype(jnp.bfloat16)
    proj = lax.all_to_all(proj_cols, "gx", split_axis=0, concat_axis=1, tiled=True)
    resid = stream_in.astype(jnp.float32) + proj.astype(jnp.float32)
    power = jnp.mean(resid * resid, axis=-1, keepdims=True)
    normed = (resid * lax.rsqrt(power + 1e-05) * norm_gain).astype(jnp.bfloat16)
    probs = jax.nn.softmax(route_scores, axis=-1)
    columns = []
    for expert in range(RESIDENT):
        columns.append(jnp.sum(jnp.where(route_ids == expert, probs, 0.0), axis=-1))
    weight = jnp.stack(columns, axis=-1).astype(jnp.bfloat16)
    normed_all, weight_all = (
        lax.all_gather(normed, "gx", axis=0, tiled=True),
        lax.all_gather(weight, "gx", axis=0, tiled=True),
    )
    rows_in = lax.dynamic_slice_in_dim(normed_all, model_block * block_width, block_width, 1)
    gate_view = gate_weight.reshape(RESIDENT, block_width, MSPLIT, narrow)
    up_view = up_weight.reshape(RESIDENT, block_width, MSPLIT, narrow)
    gate_part = jnp.einsum("bd,rdpc->bprc", rows_in, gate_view, preferred_element_type=jnp.float32)
    up_part = jnp.einsum("bd,rdpc->bprc", rows_in, up_view, preferred_element_type=jnp.float32)
    parts = jnp.stack([gate_part, up_part], axis=3)
    for bit in range(model_bits):
        parts = parts + partner(parts.astype(jnp.bfloat16), "gx", low_bits + bit).astype(
            parts.dtype
        )
    hidden = gated(parts)
    down_view = down_weight.reshape(RESIDENT, MSPLIT, narrow, block_width)
    scales = weight_all.astype(jnp.float32)
    result = jnp.zeros((batch, block_width), jnp.float32)
    for expert in range(RESIDENT):
        term = jnp.einsum(
            "bpc,pcn->bn",
            hidden[:, :, expert],
            down_view[expert],
            preferred_element_type=jnp.float32,
        )
        result = result + scales[:, expert][:, None] * term
    partial_out = result.reshape(members, seqs, block_width)
    got = lax.all_to_all(
        partial_out.astype(jnp.bfloat16), "gx", split_axis=0, concat_axis=0, tiled=True
    ).astype(partial_out.dtype)
    got = jnp.sum(got.reshape(MSPLIT, hsplit, seqs, block_width), axis=1)
    ffn = got.transpose(1, 0, 2).reshape(seqs, width)
    return (resid + ffn).astype(jnp.bfloat16)


def lane_iota(shape):
    return lax.broadcasted_iota(jnp.int32, shape, len(shape) - 1)


def row_iota(shape):
    return lax.broadcasted_iota(jnp.int32, shape, 0)


def split_three(value):
    high = value.astype(jnp.bfloat16)
    rest = value - high.astype(jnp.float32)
    mid = rest.astype(jnp.bfloat16)
    low = (rest - mid.astype(jnp.float32)).astype(jnp.bfloat16)
    return high, mid, low


def three_rows(line):
    rows = row_iota((8, HS))
    tail = jnp.zeros((8, HS), jnp.float32)
    for at, part in enumerate(split_three(line)):
        tail = jnp.where(rows == at, part.astype(jnp.float32), tail)
    return tail.astype(jnp.bfloat16)


def one_block(kernel, outs, args, spaces, scratch=(), flops=0, grant=3 << 20):
    return pl.pallas_call(
        kernel,
        out_shape=[jax.ShapeDtypeStruct(shape, dtype) for shape, dtype in outs],
        in_specs=[pl.BlockSpec(memory_space=space) for space in spaces],
        out_specs=[pl.BlockSpec(memory_space=pltpu.VMEM) for _ in outs],
        scratch_shapes=list(scratch),
        cost_estimate=pl.CostEstimate(flops=flops, transcendentals=0, bytes_accessed=1 << 20),
        compiler_params=pltpu.CompilerParams(vmem_limit_bytes=grant),
    )(*args)


def attend_kernel(*refs):
    lengths, sources, out, places, sems, work = refs[0], refs[1:9], refs[9], refs[10:18], refs[18], refs[19:]
    copies = [
        pltpu.make_async_copy(source, place, sems.at[i])
        for i, (source, place) in enumerate(zip(sources, places))
    ]
    for copy in (copies[6], copies[2], *copies[3:6], copies[0], copies[1], copies[7]):
        copy.start()
    for copy in copies[2:6]:
        copy.wait()
    ids, scores_in, query, key_new, value_new, stream, keys, values = places
    q_rows, s_rows, own_k, own_v, s_acc = work
    blocks, rows = out.shape[0], out.shape[1]
    group = NH // KVH
    for head in range(NH):
        q_rows[head : head + 1, :] = query[0:1, head * HS : (head + 1) * HS].astype(jnp.float32)
    for tile in range(s_rows.shape[0]):
        s_rows[tile : tile + 1, :] = stream[0:1, tile * HS : (tile + 1) * HS].astype(jnp.float32)
    for g in range(KVH):
        cut = slice(g * HS, (g + 1) * HS)
        here = slice(g * group, (g + 1) * group)
        own_k[here, :] = jnp.broadcast_to(key_new[0:1, cut].astype(jnp.float32), (group, HS))
        own_v[here, :] = jnp.broadcast_to(value_new[0:1, cut].astype(jnp.float32), (group, HS))
    copies[6].wait()
    for g in range(KVH):
        cut = slice(g * HS, (g + 1) * HS)
        here = slice(g * group, (g + 1) * group)
        s_acc[here, :] = lax.dot_general(
            q_rows[here, :].astype(jnp.bfloat16),
            keys[0, :, cut],
            (((1,), (1,)), ((), ())),
            preferred_element_type=jnp.float32,
        )
    scale = HS ** (-0.5)
    scores = s_acc[...] * scale
    scores = jnp.where(lane_iota(scores.shape) < lengths[0], scores, -1e30)
    own = jnp.sum(q_rows[...] * own_k[...], axis=-1, keepdims=True) * scale
    top = jnp.maximum(jnp.max(scores, axis=-1, keepdims=True), own)
    e_cache = jnp.exp(scores - top)
    e_own = jnp.exp(own - top)
    total = jnp.sum(e_cache, axis=-1, keepdims=True) + e_own
    p_cache = e_cache / total
    p_own = (e_own / total).astype(jnp.bfloat16).astype(jnp.float32)
    s_acc[...] = p_cache
    for copy in (copies[0], copies[1], copies[7]):
        copy.wait()
    for g in range(KVH):
        cut = slice(g * HS, (g + 1) * HS)
        here = slice(g * group, (g + 1) * group)
        mixed = jnp.dot(
            s_acc[here, :].astype(jnp.bfloat16), values[0, :, cut], preferred_element_type=jnp.float32
        )
        q_rows[here, :] = mixed + p_own[here, :] * own_v[here, :]
    attn = q_rows[...].astype(jnp.bfloat16)
    first = jnp.full((8, HS), scores_in[0, 0])
    second = jnp.full((8, HS), scores_in[0, 1])
    peak = jnp.maximum(first, second)
    e_first = jnp.exp(first - peak)
    e_second = jnp.exp(second - peak)
    both = e_first + e_second
    tail = jnp.zeros((8, HS), jnp.float32)
    for expert in range(RESIDENT):
        w = jnp.where(ids[0, 0] == expert, e_first / both, 0.0)
        w = w + jnp.where(ids[0, 1] == expert, e_second / both, 0.0)
        tail = jnp.where(row_iota(tail.shape) == expert, w, tail)
    tail = tail.astype(jnp.bfloat16)
    per = s_rows.shape[0] // blocks
    for block in range(blocks):
        out[block, 0:NH, :] = attn
        out[block, NH : NH + per, :] = s_rows[block * per : (block + 1) * per, :].astype(jnp.bfloat16)
        out[block, NH + per : rows, :] = tail


def project_kernel(weight, here, there, gain, out, resid_out, place_out, pick_out, rows32, lhs, acc, scaled, *, slots):
    batch, width = acc.shape
    chips, rows = here.shape[:2]
    place = lax.axis_index("gx")
    half = place % 2
    for source, core in ((here, half), (there, 1 - half)):
        first = pl.multiple_of(core * (chips * rows), 8)
        rows32[pl.ds(first, chips * rows), :] = source[...].reshape(chips * rows, HS).astype(jnp.float32)
    for head in range(NH):
        lhs[:, head * HS : (head + 1) * HS] = rows32[pl.ds(head, batch, stride=rows), :].astype(jnp.bfloat16)
    acc[...] = jnp.dot(lhs[...], weight[...], preferred_element_type=jnp.float32)
    per = width // HS
    power = jnp.zeros((batch, 1), jnp.float32)
    for q in range(per):
        cut = slice(q * HS, (q + 1) * HS)
        stream = rows32[pl.ds(NH + half * per + q, batch, stride=rows), :]
        resid = stream + acc[:, cut].astype(jnp.bfloat16).astype(jnp.float32)
        resid_out[:, cut] = resid
        power = power + jnp.sum(resid * resid, axis=-1, keepdims=True)
        scaled[:, cut] = (resid * gain[pl.ds(place * per + q, 1), :]).astype(jnp.bfloat16)
    lanes = lane_iota((batch, HS))
    eye = lanes == row_iota((batch, HS))
    out[RESIDENT * 16 :, :] = jnp.zeros((8, width), jnp.bfloat16)
    out[RESIDENT * 16 :, :HS] = three_rows(jnp.sum(jnp.where(eye, power, 0.0), axis=0, keepdims=True))
    tri = (lane_iota((batch, batch)) < row_iota((batch, batch))).astype(jnp.bfloat16)
    onehot = jnp.zeros((batch, HS), jnp.float32)
    picked = jnp.zeros((batch, HS), jnp.float32)
    for expert in range(RESIDENT):
        w = rows32[pl.ds(NH + 2 * per + expert, batch, stride=rows), :]
        named = w > 0.0
        rank = jnp.dot(tri, named.astype(jnp.bfloat16), preferred_element_type=jnp.float32)
        slot = lanes.astype(jnp.float32)
        for turn, low_edge in enumerate((expert * 16 + expert * slots % 8, 32 + expert * slots)):
            inside = (lanes >= low_edge) & (lanes < low_edge + slots)
            hit = inside & named & (rank + float(low_edge) == slot)
            onehot = jnp.where(hit, 1.0, onehot)
            if turn == 0:
                picked = jnp.where(hit, w, picked)
    hot = onehot.astype(jnp.bfloat16)
    over = (((0,), (0,)), ((), ()))
    spread = lax.dot_general(hot[:, : RESIDENT * 16], scaled[...], over, preferred_element_type=jnp.float32)
    out[: RESIDENT * 16, :] = spread.astype(jnp.bfloat16)
    hot_rows = hot[:, 32 : 32 + place_out.shape[0]]
    place_out[...] = lax.dot_general(hot_rows, eye.astype(jnp.bfloat16), over, preferred_element_type=jnp.float32)
    pick_out[...] = picked


def merged(left, right):
    return jnp.concatenate([left[:8], left[8:] + right[:8], right[8:]], axis=0)


class UpBlocks:
    def __init__(self, up, ring, sems, side):
        self.up, self.ring, self.sems, self.side = up, ring, sems, side
        self.depth, self.rows, self.narrow = ring.shape
        self.pieces = up.shape[1] // self.rows
        self.total = 4 * RESIDENT * self.pieces
        for k in range(self.depth):
            self.copy(k).start()

    def columns(self, z, side):
        return pl.ds(pl.multiple_of((2 * z + side) * self.narrow, HS), self.narrow)

    def copy(self, k):
        slot = k % self.depth
        block, piece = k // self.pieces, k % self.pieces
        source = self.up.at[
            block % RESIDENT,
            piece * self.rows : (piece + 1) * self.rows,
            self.columns(block // RESIDENT, self.side),
        ]
        return pltpu.make_async_copy(source, self.ring.at[slot], self.sems.at[slot])

    def times(self, lhs, z, expert):
        result = None
        for piece in range(self.pieces):
            k = (z * RESIDENT + expert) * self.pieces + piece
            self.copy(k).wait()
            cut = slice(piece * self.rows, (piece + 1) * self.rows)
            term = jnp.dot(lhs[expert, :, cut], self.ring[k % self.depth], preferred_element_type=jnp.float32)
            result = term if result is None else result + term
            if k + self.depth < self.total:
                self.copy(k + self.depth).start()
        return result


def stacked(work, gate, up, half):
    work[0:half, :] = gate[:half]
    work[half : 2 * half, :] = up[:half]


def both_sides(side, function):
    for fixed in range(2):
        pl.when(side == fixed)(functools.partial(function, fixed))


def side_sums(blocks, lhs, gate, z, side, slots, work):
    columns = slice((2 * z + side) * blocks.narrow, (2 * z + side + 1) * blocks.narrow)
    gates = [
        jnp.dot(lhs[expert], gate[expert, :, columns], preferred_element_type=jnp.float32) for expert in range(RESIDENT)
    ]
    ups = [blocks.times(lhs, z, expert) for expert in range(RESIDENT)]
    stacked(work, merged(*gates), merged(*ups), RESIDENT * slots)


def far_kernel(mine, other, gate, up, out, lhs_out, tail_out, ring, sems, work, *, slots):
    place = lax.axis_index("gx")
    side = place // 2 % 2
    blocks = UpBlocks(up, ring, sems, 1 - side)
    lines = 2 * RESIDENT * slots
    width = mine.shape[1]

    def join(fixed):
        for expert in range(RESIDENT):
            for at, source in ((fixed, mine), (1 - fixed, other)):
                lhs_out[expert, :, at * width : (at + 1) * width] = source[expert * 16 : (expert + 1) * 16, :]

    both_sides(place % 2, join)
    power = mine[RESIDENT * 16 :, :HS].astype(jnp.float32) + other[RESIDENT * 16 :, :HS].astype(jnp.float32)
    tail = three_rows(jnp.sum(power, axis=0, keepdims=True))
    tail_out[...] = tail.astype(jnp.float32)

    def run(fixed):
        for z in range(out.shape[0]):
            out[z, out.shape[1] - 8 :, :] = tail
            side_sums(blocks, lhs_out, gate, z, fixed, slots, work)
            for q in range(blocks.narrow // HS):
                value = work[:, q * HS : (q + 1) * HS]
                out[z, q * lines : (q + 1) * lines, :] = value.astype(jnp.bfloat16)

    both_sides(1 - side, run)


def near_kernel(lhs, tail, gate, up, out, ring, sems, work, *, slots):
    side = lax.axis_index("gx") // 2 % 2
    blocks = UpBlocks(up, ring, sems, side)
    lines = 2 * RESIDENT * slots

    def run(fixed):
        for z in range(out.shape[0]):
            out[z, out.shape[1] - 8 :, :] = tail[...]
            side_sums(blocks, lhs, gate, z, fixed, slots, work)
            for q in range(blocks.narrow // HS):
                out[z, q * lines : (q + 1) * lines, :] = work[:, q * HS : (q + 1) * HS]

    both_sides(side, run)


def pair_kernel(near_sums, got, keep, *sends):
    z = lax.axis_index("gx") // 4
    keep[...] = near_sums[z] + got[z].astype(jnp.float32)
    for d, send in enumerate(sends, 1):
        send[...] = (near_sums[z ^ d] + got[z ^ d].astype(jnp.float32)).astype(jnp.bfloat16)


def gated_kernel(keep, first, second, third, place, out, work, packed, *, slots, width):
    lines = 2 * RESIDENT * slots
    per = (keep.shape[0] - 8) // lines
    total = keep[...]
    for got in (first, second, third):
        total = total + got[...].astype(jnp.float32)
    work[...] = total
    line = jnp.sum(work[per * lines : per * lines + 8, :], axis=0, keepdims=True)
    inverse = lax.rsqrt(line / width + 1e-05)
    factor = jnp.sum(place[...] * inverse, axis=-1, keepdims=True)
    half = RESIDENT * slots
    scale = factor[:half, :]
    packed[packed.shape[0] - 8 :, :] = jnp.zeros((8, HS), jnp.float32)
    for q in range(per):
        gate = work[q * lines : q * lines + half, :] * scale
        up = work[q * lines + half : (q + 1) * lines, :] * scale
        packed[q * half : (q + 1) * half, :] = gate / (1.0 + jnp.exp(-gate)) * up
    out[...] = packed[...].astype(jnp.bfloat16)


def gather_kernel(own, first, second, third, out):
    for d, value in enumerate((own, first, second, third)):
        out[d] = value[...]


def down_side(hidden, down, side, rows32, lhs, acc, slots):
    own = lax.axis_index("gx") // 4
    each = RESIDENT * slots
    narrow = lhs.shape[3]
    for z in range(4):
        rows32[z] = hidden[z ^ own].astype(jnp.float32)
        for q in range(narrow // HS):
            for expert in range(RESIDENT):
                start = q * each + expert * slots // 8 * 8
                piece = rows32[z, start : start + 16, :]
                lhs[z, expert, :, q * HS : (q + 1) * HS] = piece.astype(jnp.bfloat16)

    def run(fixed):
        for expert in range(RESIDENT):
            total = None
            for z in range(4):
                cut = slice((2 * z + fixed) * narrow, (2 * z + fixed + 1) * narrow)
                term = jnp.dot(lhs[z, expert], down[expert, cut, :], preferred_element_type=jnp.float32)
                total = term if total is None else total + term
            acc[expert * 16 : (expert + 1) * 16, :] = total

    both_sides(side, run)


def down_near_kernel(hidden, down, acc, rows32, lhs, *, slots):
    down_side(hidden, down, lax.axis_index("gx") // 2 % 2, rows32, lhs, acc, slots)


def down_far_kernel(hidden, down, near_acc, picked, resid, out, spread, rows32, lhs, acc, *, slots):
    down_side(hidden, down, 1 - lax.axis_index("gx") // 2 % 2, rows32, lhs, acc, slots)
    half = lax.axis_index("gx") % 2
    blocks = 8
    acc[...] = acc[...] + near_acc[...]
    weight = picked[...].astype(jnp.bfloat16)[:, : RESIDENT * 16]
    result = None
    for part in split_three(acc[...]):
        term = jnp.dot(weight, part, preferred_element_type=jnp.float32)
        result = term if result is None else result + term
    own = resid[...]
    none = jnp.zeros_like(own)
    result = result + jnp.concatenate(
        [jnp.where(half == 0, own, none), jnp.where(half == 0, none, own)], axis=1
    )
    tiles = result.shape[1] // HS
    for q in range(tiles):
        for h in range(2):
            spread[pl.ds(h * tiles + q, blocks, stride=2 * tiles), :] = result[
                h * blocks : (h + 1) * blocks, q * HS : (q + 1) * HS
            ]
    out[...] = spread[...].reshape(out.shape).astype(jnp.bfloat16)


def finish_kernel(got, out):
    blocks = got.shape[0] // 2
    per = got.shape[1]
    for block in range(blocks):
        total = got[2 * block].astype(jnp.float32) + got[2 * block + 1].astype(jnp.float32)
        for q in range(per):
            at = (block * per + q) * HS
            out[0:1, at : at + HS] = total[q : q + 1, :].astype(jnp.bfloat16)


HG = 0


def fast_on_device(
    stream_in,
    query,
    key_new,
    value_new,
    key_cache,
    value_cache,
    lengths,
    route_ids,
    route_scores,
    out_weight,
    norm_gain,
    gate_weight,
    up_weight,
    down_weight,
):
    width = stream_in.shape[1]
    members = lax.axis_size("gx")
    batch = members
    own_width = width // members
    block_width = width // MSPLIT
    hidden_cols = gate_weight.shape[2]
    slots = 5 * batch // 8
    lines = 2 * RESIDENT * slots
    bf16, f32 = jnp.bfloat16, jnp.float32
    chips = [[2 * chip + core for chip in range(MSPLIT)] for core in range(2)]
    swap = [(i, i ^ 1) for i in range(members)]
    V = pltpu.VMEM

    def near(value):
        return pltpu.with_memory_space_constraint(value, V)

    rows = NH + block_width // HS + 8

    def exchange(value, groups):
        return lax.all_to_all(
            value, "gx", split_axis=0, concat_axis=0, tiled=True, axis_index_groups=groups
        )

    loaded = (route_ids, route_scores, query, key_new, value_new, stream_in, key_cache, value_cache)
    (sent,) = one_block(
        attend_kernel,
        [((MSPLIT, rows, HS), bf16)],
        [lengths] + [pltpu.with_memory_space_constraint(value, pltpu.HBM) for value in loaded],
        [pltpu.SMEM] + [pltpu.HBM] * len(loaded),
        scratch=[(pltpu.SMEM if i < 2 else pltpu.VMEM)(value.shape, value.dtype) for i, value in enumerate(loaded)]
        + [pltpu.SemaphoreType.DMA((len(loaded),))]
        + [
            pltpu.VMEM((NH, HS), f32),
            pltpu.VMEM((width // HS, HS), f32),
            pltpu.VMEM((NH, HS), f32),
            pltpu.VMEM((NH, HS), f32),
            pltpu.VMEM((NH, HS), f32),
        ],
        flops=HINT,
    )
    chip_rows = exchange(sent, chips)
    other_rows = lax.ppermute(chip_rows, "gx", swap)
    held = -(-RESIDENT * slots // 8) * 8
    mine, resid, place, picked = one_block(
        functools.partial(project_kernel, slots=slots),
        [((RESIDENT * 16 + 8, own_width), bf16), ((batch, own_width), f32), ((held, HS), f32), ((batch, HS), f32)],
        (near(out_weight), chip_rows, other_rows, norm_gain.reshape(width // HS, HS)),
        [V, V, V, V],
        scratch=[
            pltpu.VMEM((batch * rows, HS), f32),
            pltpu.VMEM((batch, width), bf16),
            pltpu.VMEM((batch, own_width), f32),
            pltpu.VMEM((batch, own_width), bf16),
        ],
    )
    other = lax.ppermute(mine, "gx", swap)
    narrow = hidden_cols // MSPLIT
    per = narrow // HS
    chunk = (per * lines + 8, HS)
    flat = (-(-per * RESIDENT * slots // 8) * 8, HS)
    up_hbm = pltpu.with_memory_space_constraint(up_weight, pltpu.HBM)

    def side_scratch(depth):
        return [
            pltpu.VMEM((depth, block_width // 2, narrow), bf16),
            pltpu.SemaphoreType.DMA((depth,)),
            pltpu.VMEM((lines, narrow), f32),
        ]

    far, lhs, tail = one_block(
        functools.partial(far_kernel, slots=slots),
        [((4,) + chunk, bf16), ((RESIDENT, 16, block_width), bf16), ((8, HS), f32)],
        (near(mine), near(other), near(gate_weight), up_hbm),
        [V, V, V, pltpu.HBM],
        scratch=side_scratch(6),
        grant=7 << 20,
    )
    crossed = lax.ppermute(far, "gx", [(i, i ^ 2) for i in range(members)])
    (near_sums,) = one_block(
        functools.partial(near_kernel, slots=slots),
        [((4,) + chunk, f32)],
        (lhs, tail, near(gate_weight), up_hbm),
        [V, V, V, pltpu.HBM],
        scratch=side_scratch(6),
        grant=7 << 20,
    )
    keep, *sends = one_block(
        pair_kernel, [(chunk, f32)] + [(chunk, bf16)] * 3, (near_sums, crossed), [V, V], flops=HINT // 5
    )
    got = []
    for d in (1, 2, 3):
        got.append(lax.ppermute(sends[d - 1], "gx", [(i, i ^ 4 * d) for i in range(members)]))
    (hidden,) = one_block(
        functools.partial(gated_kernel, slots=slots, width=width),
        [(flat, bf16)],
        (keep, *got, place),
        [V] * 5,
        scratch=[pltpu.VMEM(chunk, f32), pltpu.VMEM(flat, f32)],
        flops=HINT // 5,
    )
    parts = []
    for d in (1, 2, 3):
        parts.append(lax.ppermute(hidden, "gx", [(i, i ^ 4 * d) for i in range(members)]))
    (near_hidden,) = one_block(gather_kernel, [((4,) + flat, bf16)], (hidden, *parts), [V] * 4, flops=HG)
    far_hidden = lax.ppermute(near_hidden, "gx", [(i, i ^ 2) for i in range(members)])
    side_rows = [pltpu.VMEM((4,) + flat, f32), pltpu.VMEM((4, RESIDENT, 16, narrow), bf16)]
    sums = (RESIDENT * 16, block_width)
    (near_acc,) = one_block(
        functools.partial(down_near_kernel, slots=slots),
        [(sums, f32)],
        (near_hidden, near(down_weight)),
        [V, V],
        scratch=side_rows,
    )
    (partial_out,) = one_block(
        functools.partial(down_far_kernel, slots=slots),
        [((members, block_width // HS, HS), bf16)],
        (far_hidden, near(down_weight), near_acc, picked, resid),
        [V] * 5,
        scratch=[pltpu.VMEM((members * block_width // HS, HS), f32)] + side_rows + [pltpu.VMEM(sums, f32)],
    )
    last = exchange(partial_out, None)
    (out,) = one_block(finish_kernel, [((1, width), bf16)], (last,), [V])
    return out


def fits(shapes, members):
    width = shapes[0][1]
    hidden_cols = shapes[11][2]
    return (
        members == 2 * MSPLIT
        and shapes[0][0] == 1
        and shapes[4][1] == HS
        and width == NH * HS
        and width % (members * HS) == 0
        and hidden_cols % (MSPLIT * HS) == 0
        and (5 * members) % 8 == 0
        and 8 <= 5 * members // 8 <= 14
        and RESIDENT == 2
    )


def on_device(*args):
    if fits([arg.shape for arg in args], lax.axis_size("gx")):
        return fast_on_device(*args)
    return plain_on_device(*args)


def solution(mesh):
    return jax.shard_map(
        on_device,
        mesh=mesh,
        in_specs=(
            P(("groups", "gx"), None),
            P(("groups", "gx"), None),
            P(("groups", "gx"), None),
            P(("groups", "gx"), None),
            P(("groups", "gx"), None, None),
            P(("groups", "gx"), None, None),
            P(("groups", "gx")),
            P(("groups", "gx"), None),
            P(("groups", "gx"), None),
            P(None, "gx"),
            P(),
            P(None, "gx", None),
            P(None, "gx", None),
            P(None, "gx", None),
        ),
        out_specs=P(("groups", "gx"), None),
        check_vma=False,
    )
```
